32 devices in a mesh: gx: 8 (over z, y), gy: 4 (over x, core).
Axes of the slice: x: 2, y: 2, z: 4, core: 2. Of those that a mesh axis runs over, the one named last changes fastest.
Arguments:
- velocity_u: float32 [512, 16, 2048], P('gx', None, 'gy'), may hold values from -6 to 6
- wall_strain: float32 [512, 16, 2048], P('gx', None, 'gy'), may hold values from -6 to 6
- damping: float32 [16, 2048], P(None, 'gy'), may hold values from 0.88 to 1
Outputs:
- second_deriv: float32 [512, 16, 2048], P('gx', None, 'gy')
- cosine_coeffs: float32 [512, 16, 2048], P('gx', None, 'gy')
- pressure: float32 [512, 16, 2048], P('gx', None, 'gy')
The draws below stay inside these ranges and needn't reach their ends.
All inputs are finite; a program needn't handle non-finite values.
Results may differ from the reference program's by a relative error of at most 0.0003.
Values sent between devices are 32-bit elements; how exact they have to be, the bound alone decides.
No kernel may reach another device: no remote copies, remote signals or barrier semaphores. Data moves between devices by JAX's collectives and lax.ppermute only.
A program may use at most 128 MiB of HBM per device.

```python
import math
import jax
import jax.numpy as jnp
from jax import lax

NZ = 16
NY = 2048
NX = 512


def draw_wall_strain(key, part):
    rough_key = jax.random.fold_in(key, 0)
    return jnp.clip(jax.random.normal(rough_key, (NX, NZ, NY), jnp.float32), -6.0, 6.0)


def draw_damping(key, part):
    choose_key, long_key, short_key = jax.random.split(key, 3)
    long_share = 0.5
    long_length = jnp.exp(jax.random.uniform(long_key, (NZ, NY), jnp.float32, math.log(0.45 * NX), math.log(0.9 * NX)))
    short_length = jnp.exp(jax.random.uniform(short_key, (NZ, NY), jnp.float32, math.log(8.0), math.log(0.45 * NX)))
    chosen = jax.random.uniform(choose_key, (NZ, NY), jnp.float32) < long_share
    length = jnp.where(chosen, long_length, short_length)
    return jnp.exp(-1.0 / length)


def level_of(stream_key, dims, cuts, least, top_value):
    gain = 1.0
    for dim, parts in cuts:
        steps = jax.random.uniform(jax.random.fold_in(jax.random.fold_in(stream_key, 6), dim), (parts,), jnp.float32, least / len(cuts), top_value / len(cuts))
        gain = gain * jnp.repeat(jnp.exp(steps), dims[dim] // parts).reshape((-1,) + (1,) * (len(dims) - 1 - dim))
    return gain


def centred(stream_key, shape, width, reach, cuts=(), kind=jnp.bfloat16):
    gain = level_of(stream_key, shape, cuts, -0.22, 0.18) if cuts else 1.0
    result = jax.random.normal(stream_key, shape, jnp.float32) * width * gain
    return jnp.minimum(jnp.maximum(result, -reach), reach).astype(kind)


def setup_inputs(seed: int = 0) -> dict:
    key_list = jax.random.split(jax.random.key(seed), 4)
    return {
        "velocity_u": centred(key_list[0], (NX, NZ, NY), 1.0, 6.0, ((0, 8), (2, 4)), jnp.float32),
        "wall_strain": draw_wall_strain(jax.random.fold_in(key_list[3], 71), 0),
        "damping": draw_damping(jax.random.fold_in(key_list[3], 71), 0),
    }


def reference(velocity_u, wall_strain, damping):
    padded = jnp.pad(velocity_u, ((3, 3), (0, 0), (0, 0)))

    def shifted(offset):
        return padded[3 + offset:3 + offset + NX]
    first_deriv = 0.75 * (shifted(1) - shifted(-1)) - 3.0 / 20.0 * (shifted(2) - shifted(-2)) + 1.0 / 60.0 * (shifted(3) - shifted(-3))
    second_deriv = 1.5 * (shifted(1) + shifted(-1)) - 3.0 / 20.0 * (shifted(2) + shifted(-2)) + 1.0 / 90.0 * (shifted(3) + shifted(-3)) - 49.0 / 18.0 * shifted(0)
    divergence = first_deriv + wall_strain
    samples = jnp.arange(NY, dtype=jnp.int32)
    phase = (samples[:, None] * 2 + 1) * samples[None, :] % (4 * NY)
    table = jnp.sqrt(jnp.float32(2.0 / NY)) * jnp.cos(jnp.float32(jnp.pi) * phase.astype(jnp.float32) / (2.0 * NY))
    flat = divergence.reshape(-1, NY)
    cosine_coeffs = jnp.dot(flat, table, precision=lax.Precision.HIGHEST, preferred_element_type=jnp.float32).reshape(divergence.shape)
    weight = ((1.0 - damping) * (1.0 + damping)) ** 1.5
    forcing = weight[None, :, :] * cosine_coeffs

    def forward_step(carry, row):
        value = row + damping * carry
        return (value, value)
    zeros_plane = jnp.zeros((NZ, NY), jnp.float32)
    _, forward_sum = lax.scan(forward_step, zeros_plane, forcing)

    def backward_step(carry, row):
        value = row + damping * carry
        return (value, value)
    _, pressure = lax.scan(backward_step, zeros_plane, forward_sum, reverse=True)
    return (second_deriv, cosine_coeffs, pressure)
```

```python
import functools
import math

import jax
import jax.numpy as jnp
from jax import lax
from jax.experimental import pallas as pl
from jax.experimental.pallas import tpu as pltpu
from jax.sharding import PartitionSpec as P


LANES = 128
ROWS = 16
REACH = 3
F32 = jnp.float32
BF16 = jnp.bfloat16
VMEM_LIMIT = 48 * 1024 * 1024


def params():
    return pltpu.CompilerParams(vmem_limit_bytes=VMEM_LIMIT)


def vmem(count):
    return [pl.BlockSpec(memory_space=pltpu.VMEM)] * count


def smem(count):
    return [pl.BlockSpec(memory_space=pltpu.SMEM)] * count


def partner(x, axis, bit):
    count = lax.axis_size(axis)
    return lax.ppermute(x, axis, [(i, i ^ bit) for i in range(count)])


def halos(u):
    cells = u.shape[0]
    count, index = lax.axis_size("gx"), lax.axis_index("gx")
    even = index % 2 == 0

    def edge(last):
        start = jnp.where(last, cells - REACH, 0)
        return lax.dynamic_slice_in_dim(u, start, REACH, 0)

    first_pairs = [(i, i ^ 1) for i in range(count)]
    inner = [(i, i + 1) for i in range(1, count - 1, 2)]
    second_pairs = inner + [(b, a) for a, b in inner]
    near = lax.ppermute(edge(even), "gx", first_pairs)
    far = lax.ppermute(edge(~even), "gx", second_pairs)
    return near, far


def stencil_kernel(fold, idx, u, wall, near, far, damping, *refs):
    second, own, sends, pad = refs[0], refs[1], refs[2:-1], refs[-1]
    cells = u.shape[0]
    sub = cells // fold
    half = sub // 2
    me = idx[0]
    even = idx[1] % 2 == 0
    pad[pl.ds(REACH, cells)] = u[...]
    pad[pl.ds(0, REACH)] = jnp.where(even, far[...], near[...])
    pad[pl.ds(REACH + cells, REACH)] = jnp.where(even, near[...], far[...])

    def point(i):
        c = [pad[i + k] for k in range(2 * REACH + 1)]
        first = 0.75 * (c[4] - c[2]) - 3.0 / 20.0 * (c[5] - c[1]) + 1.0 / 60.0 * (c[6] - c[0])
        second[i] = (
            1.5 * (c[4] + c[2])
            - 3.0 / 20.0 * (c[5] + c[1])
            + 1.0 / 90.0 * (c[6] + c[0])
            - 49.0 / 18.0 * c[3]
        )
        return first + wall[i]

    for r in range(fold):
        start = (me ^ r) * sub
        for h in range(2):
            def step(j, _, r=r, h=h, start=start):
                value = point(start + h * half + j)
                if r == 0:
                    own[h * half + j] = value
                else:
                    sends[2 * (r - 1) + h][j] = value
                return 0
            lax.fori_loop(0, half, step, 0)
        if r > 0:
            sends[2 * (r - 1)][half] = damping[...]


def stencil(fold, idx, u, wall, near, far, damping):
    cells, planes, cols = u.shape
    sub = cells // fold
    half = sub // 2
    shape = lambda n: jax.ShapeDtypeStruct((n, planes, cols), F32)
    outs = [shape(cells), shape(sub)]
    for _ in range(fold - 1):
        outs += [shape(half + 1), shape(half)]
    return pl.pallas_call(
        functools.partial(stencil_kernel, fold),
        out_shape=outs,
        in_specs=smem(1) + vmem(5),
        out_specs=vmem(len(outs)),
        scratch_shapes=[pltpu.VMEM((cells + 2 * REACH, planes, cols), F32)],
        compiler_params=params(),
        cost_estimate=pl.CostEstimate(flops=cells * planes * cols * 20, bytes_accessed=cells * planes * cols * 16, transcendentals=0),
        name="stencil",
    )(idx, u, wall, near, far, damping)


def table_kernel(total, cols, fold, idx, *outs):
    rows, width = outs[0].shape
    me = idx[0]
    base = pl.program_id(0) * rows
    block = base // cols
    chunk = 64

    def tile(i, _):
        at = i * chunk
        row = lax.broadcasted_iota(jnp.int32, (chunk, LANES), 0) + (base + at - block * cols)
        sample = (row + (me ^ block) * cols).astype(F32) * 2.0 + 1.0
        lane = lax.broadcasted_iota(jnp.int32, (chunk, LANES), 1)
        modes = width // fold
        for c in range(width // LANES):
            r, rest = divmod(c * LANES, modes)
            even = ((me ^ r) * modes + rest + lane).astype(F32) * 2.0
            for parity in range(2):
                phase = sample * (even + parity)
                phase = phase - jnp.floor(phase * (1.0 / (4 * total))) * (4.0 * total)
                v = jnp.abs(phase - 2.0 * total) - total
                x = v * (math.pi / (2.0 * total))
                s = x * x
                y = -1.0 / 39916800.0
                for coefficient in (1.0 / 362880.0, -1.0 / 5040.0, 1.0 / 120.0, -1.0 / 6.0, 1.0):
                    y = y * s + coefficient
                y = y * (x * math.sqrt(2.0 / total))
                high = y.astype(BF16)
                outs[2 * parity][pl.ds(at, chunk), pl.ds(c * LANES, LANES)] = high
                outs[2 * parity + 1][pl.ds(at, chunk), pl.ds(c * LANES, LANES)] = (y - high.astype(F32)).astype(BF16)
        return 0

    lax.fori_loop(0, rows // chunk, tile, 0)


def cosine_tables(fold, idx, cols):
    total = fold * cols
    side = total // 2
    rows = min(cols, 256)
    spec = pl.BlockSpec((rows, side), lambda i: (i, 0))
    return pl.pallas_call(
        functools.partial(table_kernel, total, cols, fold),
        grid=(side // rows,),
        out_shape=[jax.ShapeDtypeStruct((side, side), BF16)] * 4,
        in_specs=smem(1),
        out_specs=[spec] * 4,
        compiler_params=params(),
        cost_estimate=pl.CostEstimate(flops=side * side * 60, bytes_accessed=side * side * 8, transcendentals=0),
        name="table",
    )(idx)


def weight_of(d):
    t = (1.0 - d) * (1.0 + d)
    return t * jnp.sqrt(t)


def lane_pick(x, index):
    return jnp.take_along_axis(x, index, axis=1)


def transform_kernel(fold, at, last, *refs):
    take = iter(refs)
    xs = [next(take) for _ in range(fold)]
    tables = [next(take) for _ in range(4)]
    if last:
        damp = next(take)
        earlier = next(take)
    else:
        own_damp = next(take)
    outs = [next(take) for _ in range(fold)]
    if last:
        ends = [next(take) for _ in range(fold)]
    else:
        damp = next(take)
        ends_all = next(take)
    parts = [next(take) for _ in range(4)]
    half = outs[0].shape[0]
    planes, cols = xs[1].shape[1:]
    lane = lax.broadcasted_iota(jnp.int32, (planes, LANES), 1)
    tiles = cols // LANES

    def fold_cell(j, _):
        for p in range(fold // 2):
            a, b = xs[p], xs[fold - 1 - p]
            for t in range(tiles):
                x = a[j + (at if p == 0 else 0), :, pl.ds(t * LANES, LANES)]
                y = b[j, :, pl.ds((tiles - 1 - t) * LANES, LANES)]
                y = lane_pick(y, LANES - 1 - lane)
                for parity in range(2):
                    v = x - y if parity else x + y
                    high = v.astype(BF16)
                    place = (pl.ds(pl.multiple_of(j * planes, planes), planes), pl.ds(p * cols + t * LANES, LANES))
                    parts[2 * parity][place] = high
                    parts[2 * parity + 1][place] = (v - high.astype(F32)).astype(BF16)
        return 0

    lax.fori_loop(0, half, fold_cell, 0)
    if not last:
        damp[0] = own_damp[...]
        for r in range(1, fold):
            damp[r] = xs[r][half]

    rows = half * planes
    modes = cols // 2
    wide = lax.broadcasted_iota(jnp.int32, (rows, LANES), 1)
    for r in range(fold):
        columns = pl.ds(r * modes, modes)
        sums = []
        for parity in range(2):
            high, low = parts[2 * parity][...], parts[2 * parity + 1][...]
            t_high, t_low = tables[2 * parity][:, columns], tables[2 * parity + 1][:, columns]
            dot = functools.partial(jnp.dot, preferred_element_type=F32)
            sums.append(dot(high, t_high) + dot(low, t_high) + dot(high, t_low))
        for t in range(tiles):
            source = slice((t // 2) * LANES, (t // 2 + 1) * LANES)
            index = wide // 2 + (t % 2) * (LANES // 2)
            even, odd = (lane_pick(s[:, source], index) for s in sums)
            tile = jnp.where(wide % 2 == 0, even, odd)
            outs[r][:, :, pl.ds(t * LANES, LANES)] = tile.reshape(half, planes, LANES)

    for r in range(fold):
        for t in range(tiles):
            at_lanes = pl.ds(t * LANES, LANES)
            d = damp[r, :, at_lanes]
            w = weight_of(d)
            f = jnp.zeros_like(d)
            forward = []
            for j in range(half):
                f = w * outs[r][j, :, at_lanes] + d * f
                forward.append(f)
            p = jnp.zeros_like(d)
            for j in reversed(range(half)):
                p = forward[j] + d * p
            if last:
                f0, p0 = earlier[0, r, :, at_lanes], earlier[1, r, :, at_lanes]
                power, gain = span(d, half)
                ends[r][0, :, at_lanes] = f + power * f0
                ends[r][1, :, at_lanes] = p0 + power * (p + gain * f0)
            else:
                ends_all[0, r, :, at_lanes] = f
                ends_all[1, r, :, at_lanes] = p


def transform(fold, at, last, xs, tables, extra):
    planes, cols = xs[0].shape[1:]
    half = xs[0].shape[0] // 2
    side = tables[0].shape[0]
    shape = lambda *n: jax.ShapeDtypeStruct(n, F32)
    outs = [shape(half, planes, cols)] * fold
    if last:
        outs += [shape(2, planes, cols)] * fold
    else:
        outs += [shape(fold, planes, cols), shape(2, fold, planes, cols)]
    rows = half * planes
    return pl.pallas_call(
        functools.partial(transform_kernel, fold, at, last),
        out_shape=outs,
        in_specs=vmem(len(xs) + 4 + len(extra)),
        out_specs=vmem(len(outs)),
        scratch_shapes=[pltpu.VMEM((rows, side), BF16)] * 4,
        compiler_params=params(),
        cost_estimate=pl.CostEstimate(flops=12 * rows * side * side, bytes_accessed=8 * side * side, transcendentals=0),
        name="transform_b" if last else "transform_a",
    )(*xs, *tables, *extra)


def span(d, cells):
    power, gain, length = d, d, 1
    while length < cells:
        gain = gain * (1.0 + power * power)
        power = power * power
        length *= 2
    return power, gain


def merge(mine, other, upper, power, gain):
    f_low, f_high = jnp.where(upper, other[0], mine[0]), jnp.where(upper, mine[0], other[0])
    p_low, p_high = jnp.where(upper, other[1], mine[1]), jnp.where(upper, mine[1], other[1])
    return jnp.stack([f_high + power * f_low, p_low + power * (p_high + gain * f_low)])


def entering(ends, damping, sub, axis_bits):
    me, row = axis_bits
    power, gain = span(damping, sub)
    bit = 1
    while len(ends) > 1:
        upper = (me // bit) % 2 == 1
        ends = [merge(ends[r], ends[r + 1], upper, power, gain) for r in range(0, len(ends), 2)]
        gain = gain * (1.0 + power * power)
        power = power * power
        bit *= 2
    mine = ends[0]
    one = jnp.ones_like(damping)
    start, stop, turn = one, one, jnp.zeros_like(damping)
    below, above = jnp.zeros_like(damping), jnp.zeros_like(damping)
    bit = 1
    while bit < lax.axis_size("gx"):
        upper = (row // bit) % 2 == 1
        other = partner(mine, "gx", bit)
        below = below + jnp.where(upper, start * other[0], 0.0)
        above = above + jnp.where(upper, turn * other[0], stop * (other[1] + gain * mine[0]))
        mine = merge(mine, other, upper, power, gain)
        turn = jnp.where(upper, power * turn, turn + stop * gain * power)
        start = jnp.where(upper, power * start, start)
        stop = jnp.where(upper, stop, power * stop)
        gain = gain * (1.0 + power * power)
        power = power * power
        bit *= 2
    return below, above


def solve_kernel(fold, idx, damping, below, above, *refs):
    pieces, coefficients, pressure = refs[: 2 * fold], refs[-2], refs[-1]
    cells, planes, cols = coefficients.shape
    sub = cells // fold
    half = sub // 2
    me = idx[0]
    for r in range(fold):
        for h in range(2):
            coefficients[pl.ds((me ^ r) * sub + h * half, half)] = pieces[2 * r + h][...]
    d = damping[...]
    w = weight_of(d)

    def forward(i, f):
        f = w * coefficients[i] + d * f
        pressure[i] = f
        return f

    lax.fori_loop(0, cells, forward, below[...], unroll=4)

    def backward(i, p):
        p = pressure[cells - 1 - i] + d * p
        pressure[cells - 1 - i] = p
        return p

    lax.fori_loop(0, cells, backward, above[...], unroll=4)


def solve(fold, idx, damping, below, above, pieces, cells):
    planes, cols = damping.shape
    return pl.pallas_call(
        functools.partial(solve_kernel, fold),
        out_shape=[jax.ShapeDtypeStruct((cells, planes, cols), F32)] * 2,
        in_specs=smem(1) + vmem(3 + len(pieces)),
        out_specs=vmem(2),
        compiler_params=params(),
        cost_estimate=pl.CostEstimate(flops=5 * cells * planes * cols, bytes_accessed=12 * cells * planes * cols, transcendentals=0),
        name="solve",
    )(idx, damping, below, above, *pieces)


def body(velocity_u, wall_strain, damping):
    cells, planes, cols = velocity_u.shape
    fold = lax.axis_size("gy")
    sub = cells // fold
    half = sub // 2
    me, row = lax.axis_index("gy"), lax.axis_index("gx")
    idx = jnp.stack([me, row]).astype(jnp.int32)
    near, far = halos(velocity_u)
    second, own, *sends = stencil(fold, idx, velocity_u, wall_strain, near, far, damping)
    order = list(range(fold - 1, 0, -1))
    got = {}
    for h in range(2):
        for r in order:
            got[r, h] = partner(sends[2 * (r - 1) + h], "gy", r)
    tables = cosine_tables(fold, idx, cols)
    first = transform(fold, 0, False, [own] + [got[r, 0] for r in range(1, fold)], tables, [damping])
    out_a, every_damping, ends_a = first[:fold], first[fold], first[fold + 1]
    second_part = transform(fold, half, True, [own] + [got[r, 1] for r in range(1, fold)], tables, [every_damping, ends_a])
    out_b, ends_b = second_part[:fold], second_part[fold:]
    modes = {(0, 0): out_a[0], (0, 1): out_b[0]}
    for r in order:
        modes[r, 0] = partner(out_a[r], "gy", r)
    ends = [ends_b[0]] + [partner(ends_b[r], "gy", r) for r in range(1, fold)]
    for r in order:
        modes[r, 1] = partner(out_b[r], "gy", r)
    below, above = entering(ends, damping, sub, (me, row))
    pieces = [modes[r, h] for r in range(fold) for h in range(2)]
    coefficients, pressure = solve(fold, idx, damping, below, above, pieces, cells)
    return second, coefficients, pressure


def solution(mesh):
    return jax.shard_map(
        body,
        mesh=mesh,
        in_specs=(P("gx", None, "gy"), P("gx", None, "gy"), P(None, "gy")),
        out_specs=(P("gx", None, "gy"), P("gx", None, "gy"), P("gx", None, "gy")),
        check_vma=False,
    )
```

```python
import functools
import math

import jax
import jax.numpy as jnp
from jax import lax
from jax.experimental import pallas as pl
from jax.experimental.pallas import tpu as pltpu
from jax.sharding import PartitionSpec as P


LANES = 128
REACH = 3
F32 = jnp.float32
BF16 = jnp.bfloat16
MIB = 1024 * 1024


def params(limit=16 * MIB):
    return pltpu.CompilerParams(vmem_limit_bytes=limit)


def vmem(count):
    return [pl.BlockSpec(memory_space=pltpu.VMEM)] * count


def smem(count):
    return [pl.BlockSpec(memory_space=pltpu.SMEM)] * count


def hbm(count):
    return [pl.BlockSpec(memory_space=pltpu.HBM)] * count


def partner(x, axis, bit):
    count = lax.axis_size(axis)
    return lax.ppermute(x, axis, [(i, i ^ bit) for i in range(count)])


def chunks(sub):
    later = max(sub // 4, REACH)
    return sub - later, later


def chunk_start(block, h, sub):
    first, later = chunks(sub)
    return block * sub + (jnp.where(block == 0, later, 0) if h == 0 else jnp.where(block == 0, 0, first))


def derivatives(cell, at):
    c = [cell(at + k) for k in range(2 * REACH + 1)]
    first = 0.75 * (c[4] - c[2]) - 3.0 / 20.0 * (c[5] - c[1]) + 1.0 / 60.0 * (c[6] - c[0])
    second = (
        1.5 * (c[4] + c[2])
        - 3.0 / 20.0 * (c[5] + c[1])
        + 1.0 / 90.0 * (c[6] + c[0])
        - 49.0 / 18.0 * c[3]
    )
    return first, second


def lead_kernel(fold, idx, u_in, wall_in, damping_in, *refs):
    sends, (near, far, u, wall, damping, sems) = refs[: fold - 1], refs[fold - 1 :]
    cells = u.shape[0]
    sub = cells // fold
    size = chunks(sub)[0]
    me, row = idx[0], idx[1]
    order = list(range(fold - 1, -1, -1))
    rows = {r: pl.ds((me ^ r) * sub, sub) for r in order}
    u_copies = [pltpu.make_async_copy(u_in.at[rows[r]], u.at[rows[r]], sems.at[0, r]) for r in order]
    w_copies = {r: pltpu.make_async_copy(wall_in.at[rows[r]], wall.at[rows[r]], sems.at[1, r]) for r in order}
    d_copy = pltpu.make_async_copy(damping_in, damping, sems.at[2, 0])
    for copy in u_copies:
        copy.start()
    d_copy.start()
    for r in order:
        w_copies[r].start()
    for copy in u_copies:
        copy.wait()
    even = row % 2 == 0
    near[...] = u[pl.ds(jnp.where(even, cells - REACH, 0), REACH)]
    far[...] = u[pl.ds(jnp.where(even, 0, cells - REACH), REACH)]
    d_copy.wait()
    for r in order[:-1]:
        start = chunk_start(me ^ r, 0, sub)
        w_copies[r].wait()

        def step(j, _, r=r, start=start):
            first, _ = derivatives(lambda k: u[k], start - REACH + j)
            sends[r - 1][j] = first + wall[start + j]
            return 0

        lax.fori_loop(0, size, step, 0, unroll=2)
        sends[r - 1][size] = damping[...]
    w_copies[0].wait()


def lead(fold, idx, u, wall, damping):
    cells, planes, cols = u.shape
    size = chunks(cells // fold)[0]
    shape = lambda n: jax.ShapeDtypeStruct((n, planes, cols), F32)
    outs = [shape(size + 1)] * (fold - 1) + [shape(REACH)] * 2 + [shape(cells)] * 2
    outs += [jax.ShapeDtypeStruct((planes, cols), F32)]
    return pl.pallas_call(
        functools.partial(lead_kernel, fold),
        out_shape=outs,
        in_specs=smem(1) + hbm(3),
        out_specs=vmem(len(outs)),
        scratch_shapes=[pltpu.SemaphoreType.DMA((3, fold))],
        compiler_params=params(),
        cost_estimate=pl.CostEstimate(flops=cells * planes * cols * 6, bytes_accessed=cells * planes * cols * 6, transcendentals=0),
        name="lead",
    )(idx, u, wall, damping)


def stencil_kernel(fold, idx, u, wall, near, far, second_out, *refs):
    own, sends, (pad, second, out_sems) = refs[0], refs[1:fold], refs[fold:]
    cells = u.shape[0]
    sub = cells // fold
    sizes = chunks(sub)
    me = idx[0]
    even = idx[1] % 2 == 0
    pad[pl.ds(REACH, cells)] = u[...]
    pad[pl.ds(0, REACH)] = jnp.where(even, far[...], near[...])
    pad[pl.ds(REACH + cells, REACH)] = jnp.where(even, near[...], far[...])
    out_copies = []
    for r in range(fold - 1, -1, -1):
        block = me ^ r
        for h in (1, 0):
            start = chunk_start(block, h, sub)

            def step(j, _, r=r, h=h, start=start):
                first, second[start + j] = derivatives(lambda k: pad[k], start + j)
                if r == 0:
                    own[h * sizes[0] + j] = first + wall[start + j]
                elif h == 1:
                    sends[r - 1][j] = first + wall[start + j]
                return 0

            lax.fori_loop(0, sizes[h], step, 0, unroll=2)
        rows = pl.ds(block * sub, sub)
        copy = pltpu.make_async_copy(second.at[rows], second_out.at[rows], out_sems.at[r])
        copy.start()
        out_copies.append(copy)
    for copy in out_copies:
        copy.wait()


def stencil(fold, idx, u, wall, near, far):
    cells, planes, cols = u.shape
    sub = cells // fold
    later = chunks(sub)[1]
    shape = lambda n: jax.ShapeDtypeStruct((n, planes, cols), F32)
    outs = [shape(cells), shape(sub)] + [shape(later)] * (fold - 1)
    return pl.pallas_call(
        functools.partial(stencil_kernel, fold),
        out_shape=outs,
        in_specs=smem(1) + vmem(4),
        out_specs=hbm(1) + vmem(len(outs) - 1),
        scratch_shapes=[
            pltpu.VMEM((cells + 2 * REACH, planes, cols), F32),
            pltpu.VMEM((cells, planes, cols), F32),
            pltpu.SemaphoreType.DMA((fold,)),
        ],
        compiler_params=params(),
        cost_estimate=pl.CostEstimate(flops=cells * planes * cols * 20, bytes_accessed=cells * planes * cols * 16, transcendentals=0),
        name="stencil",
    )(idx, u, wall, near, far)


def exchange_edges(near, far):
    count = lax.axis_size("gx")
    inner = [(i, i + 1) for i in range(1, count - 1, 2)]
    far = lax.ppermute(far, "gx", inner + [(b, a) for a, b in inner])
    return partner(near, "gx", 1), far


def half_turn(phase, total):
    phase = phase - jnp.floor(phase * (1.0 / (4 * total))) * (4.0 * total)
    x = (jnp.abs(phase - 2.0 * total) - total) * (math.pi / (2.0 * total))
    s = x * x
    y = -1.0 / 39916800.0
    for coefficient in (1.0 / 362880.0, -1.0 / 5040.0, 1.0 / 120.0, -1.0 / 6.0, 1.0):
        y = y * s + coefficient
    return y * x


def table_kernel(total, cols, fold, chunk, idx, *outs):
    rows, width = outs[0].shape
    me = idx[0]
    modes = width // fold
    group = 8
    whole = lambda *shape: lambda axis: lax.broadcasted_iota(jnp.int32, shape, axis)
    base, inner, outer = whole(group, LANES), whole(chunk // group, LANES), whole(rows // chunk, LANES)
    at = outer(0) * chunk
    block = at // cols
    shifts = ((me ^ block) * cols + (at - block * cols)).astype(F32) * 2.0
    steps = (inner(0) * (2 * group)).astype(F32)
    sample = base(0).astype(F32) * 2.0 + 1.0

    def both(phase):
        return half_turn(phase, total), half_turn(phase - total, total)

    def column(c, _):
        r = c * LANES // modes
        first = (me ^ r) * modes + (c * LANES - r * modes)
        for parity in range(2):
            mode = lambda iota: (first + iota(1)).astype(F32) * 2.0 + parity
            c0, s0 = (v * math.sqrt(2.0 / total) for v in both(sample * mode(base)))
            ci, si = both(steps * mode(inner))
            co, so = both(shifts * mode(outer))
            cosine = jnp.concatenate([c0 * ci[i : i + 1] - s0 * si[i : i + 1] for i in range(chunk // group)])
            sine = jnp.concatenate([s0 * ci[i : i + 1] + c0 * si[i : i + 1] for i in range(chunk // group)])
            for i in range(rows // chunk):
                y = cosine * co[i : i + 1] - sine * so[i : i + 1]
                high = y.astype(BF16)
                place = (pl.ds(i * chunk, chunk), pl.ds(pl.multiple_of(c * LANES, LANES), LANES))
                outs[2 * parity][place] = high
                outs[2 * parity + 1][place] = (y - high.astype(F32)).astype(BF16)
        return 0

    lax.fori_loop(0, width // LANES, column, 0)


def cosine_tables(fold, idx, cols):
    total = fold * cols
    side = total // 2
    return pl.pallas_call(
        functools.partial(table_kernel, total, cols, fold, 128),
        out_shape=[jax.ShapeDtypeStruct((side, side), BF16)] * 4,
        in_specs=smem(1),
        out_specs=vmem(4),
        compiler_params=params(),
        cost_estimate=pl.CostEstimate(flops=side * side * 60, bytes_accessed=side * side * 8, transcendentals=0),
        name="table",
    )(idx)


def weight_of(d):
    t = (1.0 - d) * (1.0 + d)
    return t * jnp.sqrt(t)


def lane_pick(x, index):
    return jnp.take_along_axis(x, index, axis=1)


def transform_kernel(fold, at, sizes, cuts, last, idx, *refs):
    take = iter(refs)
    xs = [next(take) for _ in range(fold)]
    tables = [next(take) for _ in range(4)]
    if last:
        damp = next(take)
        earlier = next(take)
    else:
        own_damp = next(take)
    outs = [[next(take) for _ in pieces] for pieces in cuts]
    if last:
        ends = [next(take) for _ in range(fold)]
    else:
        damp = next(take)
        ends_all = next(take)
    parts = [next(take) for _ in range(2)]
    half = sizes[last]
    planes, cols = xs[1].shape[1:]
    lane = lax.broadcasted_iota(jnp.int32, (planes, LANES), 1)
    tiles = cols // LANES

    def fold_cell(j, _):
        for p in range(fold // 2):
            a, b = xs[p], xs[fold - 1 - p]
            for t in range(tiles):
                x = a[j + (at if p == 0 else 0), :, pl.ds(t * LANES, LANES)]
                y = b[j, :, pl.ds((tiles - 1 - t) * LANES, LANES)]
                y = lane_pick(y, LANES - 1 - lane)
                for parity in range(2):
                    v = x - y if parity else x + y
                    high = v.astype(BF16)
                    columns = pl.ds(p * cols + t * LANES, LANES)
                    place = pl.multiple_of(j * planes, planes)
                    parts[parity][pl.ds(place, planes), columns] = high
                    parts[parity][pl.ds(half * planes + place, planes), columns] = (v - high.astype(F32)).astype(BF16)
        return 0

    lax.fori_loop(0, half, fold_cell, 0)
    if not last:
        damp[0] = own_damp[...]
        for r in range(1, fold):
            damp[r] = xs[r][half]

    rows = half * planes
    modes = cols // 2
    wide = lax.broadcasted_iota(jnp.int32, (rows, LANES), 1)
    for r in range(fold):
        columns = pl.ds(r * modes, modes)
        sums = []
        for parity in range(2):
            dot = functools.partial(jnp.dot, preferred_element_type=F32)
            both = dot(parts[parity][...], tables[2 * parity][:, columns])
            rest = dot(parts[parity][:rows], tables[2 * parity + 1][:, columns])
            sums.append(both[:rows] + both[rows:] + rest)
        for t in range(tiles):
            source = slice((t // 2) * LANES, (t // 2 + 1) * LANES)
            index = wide // 2 + (t % 2) * (LANES // 2)
            even, odd = (lane_pick(s[:, source], index) for s in sums)
            tile = jnp.where(wide % 2 == 0, even, odd)
            tile = tile.reshape(half, planes, LANES)
            for out, (low, high) in zip(outs[r], cuts[r]):
                out[:, :, pl.ds(t * LANES, LANES)] = tile[low:high]

    for r in range(fold):
        for t in range(tiles):
            at_lanes = pl.ds(t * LANES, LANES)
            d = damp[r, :, at_lanes]
            w = weight_of(d)
            f = jnp.zeros_like(d)
            forward = []
            for out, (low, high) in zip(outs[r], cuts[r]):
                for j in range(high - low):
                    f = w * out[j, :, at_lanes] + d * f
                    forward.append(f)
            p = jnp.zeros_like(d)
            for j in reversed(range(half)):
                p = forward[j] + d * p
            if last:
                f0, p0 = earlier[0, r, :, at_lanes], earlier[1, r, :, at_lanes]
                f, p = merge((f, p), (f0, p0), idx[0] != 0, span(d, half), span(d, sizes[0]))
                ends[r][0, :, at_lanes] = f
                ends[r][1, :, at_lanes] = p
            else:
                ends_all[0, r, :, at_lanes] = f
                ends_all[1, r, :, at_lanes] = p


def transform(fold, idx, sub, cuts, last, xs, tables, extra):
    planes, cols = xs[0].shape[1:]
    sizes = chunks(sub)
    half = sizes[last]
    at = sizes[0] if last else 0
    side = tables[0].shape[0]
    shape = lambda *n: jax.ShapeDtypeStruct(n, F32)
    outs = [shape(high - low, planes, cols) for pieces in cuts for low, high in pieces]
    if last:
        outs += [shape(2, planes, cols)] * fold
    else:
        outs += [shape(fold, planes, cols), shape(2, fold, planes, cols)]
    rows = half * planes
    return pl.pallas_call(
        functools.partial(transform_kernel, fold, at, sizes, cuts, last),
        out_shape=outs,
        in_specs=smem(1) + vmem(len(xs) + 4 + len(extra)),
        out_specs=vmem(len(outs)),
        scratch_shapes=[pltpu.VMEM((2 * rows, side), BF16)] * 2,
        compiler_params=params(),
        cost_estimate=pl.CostEstimate(flops=12 * rows * side * side, bytes_accessed=8 * side * side, transcendentals=0),
        name="transform_b" if last else "transform_a",
    )(idx, *xs, *tables, *extra)


def span(d, cells):
    power, gain, block = None, None, (d, d)
    while cells:
        if cells % 2:
            if power is None:
                power, gain = block
            else:
                power, gain = power * block[0], gain + power * power * block[1]
        block = doubled(*block)
        cells //= 2
    return power, gain


def merge(mine, other, upper, span_mine, span_other):
    pick = lambda a, b: a if a is b else jnp.where(upper, a, b)
    f_low, f_high = jnp.where(upper, other[0], mine[0]), jnp.where(upper, mine[0], other[0])
    p_low, p_high = jnp.where(upper, other[1], mine[1]), jnp.where(upper, mine[1], other[1])
    high_power, high_gain = pick(span_mine[0], span_other[0]), pick(span_mine[1], span_other[1])
    low_power = pick(span_other[0], span_mine[0])
    return f_high + high_power * f_low, p_low + low_power * (p_high + high_gain * f_low)


def doubled(power, gain):
    return power * power, gain * (1.0 + power * power)


def stages(fold, count):
    bits = [1 << k for k in range(count.bit_length() - 1)]
    groups = [[1 << k for k in range(fold.bit_length() - 1)]]
    return groups + [bits[k : k + 2] for k in range(0, len(bits), 2)]


def peers(bits):
    offsets = [0]
    for bit in bits:
        offsets += [o ^ bit for o in offsets]
    return offsets


def combine(groups, stage, d, sub, me, row, ends, entry):
    power, gain = span(d, sub)
    start, stop, turn = None, None, None
    for k, bits in enumerate(groups[: stage + 1]):
        position = row if k else me
        if k == 1:
            start, stop, turn = jnp.ones_like(d), jnp.ones_like(d), jnp.zeros_like(d)
            if entry is None:
                entry = (jnp.zeros_like(d), jnp.zeros_like(d))
        for bit in bits:
            upper = position & bit != 0
            if k:
                if k == stage:
                    mine, other = ends[0], ends[1]
                    below, above = entry
                    below = below + jnp.where(upper, start * other[0], 0.0)
                    above = above + jnp.where(upper, turn * other[0], stop * (other[1] + gain * mine[0]))
                    entry = (below, above)
                turn = jnp.where(upper, power * turn, turn + stop * gain * power)
                start = jnp.where(upper, power * start, start)
                stop = jnp.where(upper, stop, power * stop)
            if k == stage:
                ends = [merge(ends[i], ends[i + 1], upper, (power, gain), (power, gain)) for i in range(0, len(ends), 2)]
            power, gain = doubled(power, gain)
    return ends[0], entry


def combine_tiles(groups, stage, sub, idx, damping, ends, entry, put):
    for t in range(damping.shape[1] // LANES):
        at = pl.ds(t * LANES, LANES)
        pairs = [(e[0, :, at], e[1, :, at]) for e in ends]
        entered = None if entry is None else (entry[0, :, at], entry[1, :, at])
        put(at, *combine(groups, stage, damping[:, at], sub, idx[0], idx[1], pairs, entered))


def combine_kernel(groups, stage, sub, idx, damping, *refs):
    count = 1 << len(groups[stage])
    ends, rest = refs[:count], refs[count:]
    entry = rest[0] if stage > 1 else None
    outs = rest[-2:] if stage else rest[-1:]

    def put(at, union, entered):
        outs[0][0, :, at], outs[0][1, :, at] = union
        if stage:
            outs[1][0, :, at], outs[1][1, :, at] = entered

    combine_tiles(groups, stage, sub, idx, damping, ends, entry, put)


def combined(groups, stage, sub, idx, damping, ends, entry):
    pair = jax.ShapeDtypeStruct((2,) + damping.shape, F32)
    extra = [entry] if stage > 1 else []
    outs = [pair, pair] if stage else [pair]
    return pl.pallas_call(
        functools.partial(combine_kernel, groups, stage, sub),
        out_shape=outs,
        in_specs=smem(1) + vmem(1 + len(ends) + len(extra)),
        out_specs=vmem(len(outs)),
        compiler_params=params(),
        cost_estimate=pl.CostEstimate(flops=100 * damping.size, bytes_accessed=32 * damping.size, transcendentals=0),
    )(idx, damping, *ends, *extra)


def solve_kernel(fold, groups, cuts, idx, damping, *refs):
    stage = len(groups) - 1
    count = 1 << len(groups[stage])
    ends, rest = refs[:count], refs[count:]
    if stage > 1:
        entry, rest = rest[0], rest[1:]
    else:
        entry = None
    count = sum(len(c) for part in cuts for c in part)
    pieces, rest = rest[:count], rest[count:]
    coefficients_out, pressure_out, coefficients, pressure, entered, c_sems, p_sems = rest
    cells = coefficients.shape[0]
    sub = cells // fold
    half = sub // 2
    copies = []
    for h in range(2):
        for r in range(fold):
            for low, high in cuts[h][r]:
                rows = pl.ds(chunk_start(idx[0] ^ r, h, sub) + low, high - low)
                k = len(copies)
                coefficients[rows] = pieces[k][...]
                copies.append(pltpu.make_async_copy(coefficients.at[rows], coefficients_out.at[rows], c_sems.at[k]))
                copies[k].start()

    def put(at, union, entry):
        entered[0, :, at], entered[1, :, at] = entry

    combine_tiles(groups, stage, sub, idx, damping, ends, entry, put)
    d = damping[...]
    w = weight_of(d)

    def forward(i, f):
        f = w * coefficients[i] + d * f
        pressure[i] = f
        return f

    lax.fori_loop(0, cells, forward, entered[0], unroll=4)

    p = entered[1]
    for block in reversed(range(2 * fold)):

        def backward(i, p, block=block):
            at = (block + 1) * half - 1 - i
            p = pressure[at] + d * p
            pressure[at] = p
            return p

        p = lax.fori_loop(0, half, backward, p, unroll=4)
        rows = pl.ds(block * half, half)
        copies.append(pltpu.make_async_copy(pressure.at[rows], pressure_out.at[rows], p_sems.at[block]))
        copies[-1].start()
    for copy in copies:
        copy.wait()


def solve(fold, groups, cuts, idx, damping, ends, entry, pieces, cells):
    planes, cols = damping.shape
    shape = (cells, planes, cols)
    extra = [entry] if len(groups) > 2 else []
    return pl.pallas_call(
        functools.partial(solve_kernel, fold, groups, cuts),
        out_shape=[jax.ShapeDtypeStruct(shape, F32)] * 2,
        in_specs=smem(1) + vmem(1 + len(ends) + len(extra) + len(pieces)),
        out_specs=hbm(2),
        scratch_shapes=[
            pltpu.VMEM(shape, F32),
            pltpu.VMEM(shape, F32),
            pltpu.VMEM((2, planes, cols), F32),
            pltpu.SemaphoreType.DMA((len(pieces),)),
            pltpu.SemaphoreType.DMA((2 * fold,)),
        ],
        compiler_params=params(),
        cost_estimate=pl.CostEstimate(flops=5 * cells * planes * cols, bytes_accessed=12 * cells * planes * cols, transcendentals=0),
        name="solve",
    )(idx, damping, *ends, *extra, *pieces)


def body(velocity_u, wall_strain, damping):
    cells, _, cols = velocity_u.shape
    fold = lax.axis_size("gy")
    sub = cells // fold
    me, row = lax.axis_index("gy"), lax.axis_index("gx")
    idx = jnp.stack([me, row]).astype(jnp.int32)
    order = list(range(fold - 1, 0, -1))
    *sends, near, far, u, wall, damping = lead(fold, idx, velocity_u, wall_strain, damping)
    got = {(r, 0): partner(sends[r - 1], "gy", r) for r in order}
    near, far = exchange_edges(near, far)
    second, own, *sends = stencil(fold, idx, u, wall, near, far)
    for r in order:
        got[r, 1] = partner(sends[r - 1], "gy", r)
    tables = cosine_tables(fold, idx, cols)
    cuts = pieces_of(fold, sub)
    first = transform(fold, idx, sub, cuts[0], 0, [own] + [got[r, 0] for r in range(1, fold)], tables, [damping])
    every_damping, ends_a = first[-2:]
    extra = [every_damping, ends_a]
    rest = transform(fold, idx, sub, cuts[1], 1, [own] + [got[r, 1] for r in range(1, fold)], tables, extra)
    ends_b = rest[-fold:]
    pieces = []
    for h, outs in enumerate((first, rest)):
        outs = iter(outs)
        for r in range(fold):
            for _ in range(len(cuts[h][r])):
                out = next(outs)
                pieces.append(out if r == 0 else partner(out, "gy", r))
    groups = stages(fold, lax.axis_size("gx"))
    ends = [ends_b[r] if r == 0 else partner(ends_b[r], "gy", r) for r in peers(groups[0])]
    entry = None
    for stage in range(1, len(groups)):
        mine, *entries = combined(groups, stage - 1, sub, idx, damping, ends, entry)
        entry = entries[0] if entries else None
        ends = [mine] + [partner(mine, "gx", o) for o in peers(groups[stage])[1:]]
    coefficients, pressure = solve(fold, groups, cuts, idx, damping, ends, entry, pieces, cells)
    return second, coefficients, pressure


def pieces_of(fold, sub):
    first, later = chunks(sub)
    cut = first // 2
    whole = [[(0, first)] for _ in range(fold)]
    whole[fold - 1] = [(0, cut), (cut, first)]
    return whole, [[(0, later)] for _ in range(fold)]


def solution(mesh):
    return jax.shard_map(
        body,
        mesh=mesh,
        in_specs=(P("gx", None, "gy"), P("gx", None, "gy"), P(None, "gy")),
        out_specs=(P("gx", None, "gy"), P("gx", None, "gy"), P("gx", None, "gy")),
        check_vma=False,
    )
```

```python
import functools
import math

import jax
import jax.numpy as jnp
from jax import lax
from jax.experimental import pallas as pl
from jax.experimental.pallas import tpu as pltpu
from jax.sharding import PartitionSpec as P


LANES = 128
REACH = 3
F32 = jnp.float32
BF16 = jnp.bfloat16
MIB = 1024 * 1024


def params(limit=16 * MIB):
    return pltpu.CompilerParams(vmem_limit_bytes=limit)


def vmem(count):
    return [pl.BlockSpec(memory_space=pltpu.VMEM)] * count


def smem(count):
    return [pl.BlockSpec(memory_space=pltpu.SMEM)] * count


def hbm(count):
    return [pl.BlockSpec(memory_space=pltpu.HBM)] * count


def partner(x, axis, bit):
    count = lax.axis_size(axis)
    return lax.ppermute(x, axis, [(i, i ^ bit) for i in range(count)])


def chunks(sub):
    later = max(5 * sub // 16, REACH)
    return sub - later, later


def chunk_start(block, h, sub):
    first, later = chunks(sub)
    return block * sub + (jnp.where(block == 0, later, 0) if h == 0 else jnp.where(block == 0, 0, first))


def derivatives(cell, at):
    c = [cell(at + k) for k in range(2 * REACH + 1)]
    first = 0.75 * (c[4] - c[2]) - 3.0 / 20.0 * (c[5] - c[1]) + 1.0 / 60.0 * (c[6] - c[0])
    second = (
        1.5 * (c[4] + c[2])
        - 3.0 / 20.0 * (c[5] + c[1])
        + 1.0 / 90.0 * (c[6] + c[0])
        - 49.0 / 18.0 * c[3]
    )
    return first, second


def lead_kernel(fold, idx, u_in, wall_in, *refs):
    sends, (near, far, u, wall, sems) = refs[: fold - 1], refs[fold - 1 :]
    cells = u.shape[0]
    sub = cells // fold
    size = chunks(sub)[0]
    me, row = idx[0], idx[1]
    order = list(range(fold - 1, -1, -1))
    rows = {r: pl.ds((me ^ r) * sub, sub) for r in order}
    u_copies = [pltpu.make_async_copy(u_in.at[rows[r]], u.at[rows[r]], sems.at[0, r]) for r in order]
    w_copies = {r: pltpu.make_async_copy(wall_in.at[rows[r]], wall.at[rows[r]], sems.at[1, r]) for r in order}
    for copy in u_copies:
        copy.start()
    for r in order:
        w_copies[r].start()
    for copy in u_copies:
        copy.wait()
    even = row % 2 == 0
    for r in order[:-1]:
        start = chunk_start(me ^ r, 0, sub)
        w_copies[r].wait()

        def step(j, _, r=r, start=start):
            first, _ = derivatives(lambda k: u[k], start - REACH + j)
            sends[r - 1][j] = first + wall[start + j]
            return 0

        lax.fori_loop(0, size, step, 0, unroll=2)
    near[...] = u[pl.ds(jnp.where(even, cells - REACH, 0), REACH)]
    far[...] = u[pl.ds(jnp.where(even, 0, cells - REACH), REACH)]
    w_copies[0].wait()


def lead(fold, idx, u, wall):
    cells, planes, cols = u.shape
    size = chunks(cells // fold)[0]
    shape = lambda n: jax.ShapeDtypeStruct((n, planes, cols), F32)
    outs = [shape(size)] * (fold - 1) + [shape(REACH)] * 2 + [shape(cells)] * 2
    return pl.pallas_call(
        functools.partial(lead_kernel, fold),
        out_shape=outs,
        in_specs=smem(1) + hbm(2),
        out_specs=vmem(len(outs)),
        scratch_shapes=[pltpu.SemaphoreType.DMA((2, fold))],
        compiler_params=params(48 * MIB),
        cost_estimate=pl.CostEstimate(flops=cells * planes * cols * 6, bytes_accessed=cells * planes * cols * 6, transcendentals=0),
        name="lead",
    )(idx, u, wall)


def stencil_kernel(fold, idx, u, wall, near, far, second_out, *refs):
    own, sends, (pad, second, out_sems) = refs[0], refs[1:fold], refs[fold:]
    cells = u.shape[0]
    sub = cells // fold
    sizes = chunks(sub)
    me = idx[0]
    even = idx[1] % 2 == 0
    pad[pl.ds(REACH, cells)] = u[...]
    pad[pl.ds(0, REACH)] = jnp.where(even, far[...], near[...])
    pad[pl.ds(REACH + cells, REACH)] = jnp.where(even, near[...], far[...])
    out_copies = []
    for r in range(fold - 1, -1, -1):
        block = me ^ r
        for h in (1, 0):
            start = chunk_start(block, h, sub)

            def step(j, _, r=r, h=h, start=start):
                first, second[start + j] = derivatives(lambda k: pad[k], start + j)
                if r == 0:
                    own[h * sizes[0] + j] = first + wall[start + j]
                elif h == 1:
                    sends[r - 1][j] = first + wall[start + j]
                return 0

            lax.fori_loop(0, sizes[h], step, 0, unroll=2)
        rows = pl.ds(block * sub, sub)
        copy = pltpu.make_async_copy(second.at[rows], second_out.at[rows], out_sems.at[r])
        copy.start()
        out_copies.append(copy)
    for copy in out_copies:
        copy.wait()


def stencil(fold, idx, u, wall, near, far):
    cells, planes, cols = u.shape
    sub = cells // fold
    later = chunks(sub)[1]
    shape = lambda n: jax.ShapeDtypeStruct((n, planes, cols), F32)
    outs = [shape(cells), shape(sub)] + [shape(later)] * (fold - 1)
    return pl.pallas_call(
        functools.partial(stencil_kernel, fold),
        out_shape=outs,
        in_specs=smem(1) + vmem(4),
        out_specs=hbm(1) + vmem(len(outs) - 1),
        scratch_shapes=[
            pltpu.VMEM((cells + 2 * REACH, planes, cols), F32),
            pltpu.VMEM((cells, planes, cols), F32),
            pltpu.SemaphoreType.DMA((fold,)),
        ],
        compiler_params=params(),
        cost_estimate=pl.CostEstimate(flops=cells * planes * cols * 20, bytes_accessed=cells * planes * cols * 16, transcendentals=0),
        name="stencil",
    )(idx, u, wall, near, far)


def exchange_edges(near, far):
    count = lax.axis_size("gx")
    inner = [(i, i + 1) for i in range(1, count - 1, 2)]
    far = lax.ppermute(far, "gx", inner + [(b, a) for a, b in inner])
    return partner(near, "gx", 1), far


def half_turn(phase, total):
    phase = phase - jnp.floor(phase * (1.0 / (4 * total))) * (4.0 * total)
    x = (jnp.abs(phase - 2.0 * total) - total) * (math.pi / (2.0 * total))
    s = x * x
    y = -1.0 / 39916800.0
    for coefficient in (1.0 / 362880.0, -1.0 / 5040.0, 1.0 / 120.0, -1.0 / 6.0, 1.0):
        y = y * s + coefficient
    return y * x


def table_kernel(total, cols, fold, chunk, idx, *outs):
    rows, width = outs[0].shape
    me = idx[0]
    modes = width // fold
    group = 8
    whole = lambda *shape: lambda axis: lax.broadcasted_iota(jnp.int32, shape, axis)
    base, inner, outer = whole(group, LANES), whole(chunk // group, LANES), whole(rows // chunk, LANES)
    at = outer(0) * chunk
    block = at // cols
    shifts = ((me ^ block) * cols + (at - block * cols)).astype(F32) * 2.0
    steps = (inner(0) * (2 * group)).astype(F32)
    sample = base(0).astype(F32) * 2.0 + 1.0

    def both(phase):
        return half_turn(phase, total), half_turn(phase - total, total)

    def column(c, _):
        r = c * LANES // modes
        first = (me ^ r) * modes + (c * LANES - r * modes)
        for parity in range(2):
            mode = lambda iota: (first + iota(1)).astype(F32) * 2.0 + parity
            c0, s0 = (v * math.sqrt(2.0 / total) for v in both(sample * mode(base)))
            ci, si = both(steps * mode(inner))
            co, so = both(shifts * mode(outer))
            cosine = jnp.concatenate([c0 * ci[i : i + 1] - s0 * si[i : i + 1] for i in range(chunk // group)])
            sine = jnp.concatenate([s0 * ci[i : i + 1] + c0 * si[i : i + 1] for i in range(chunk // group)])
            for i in range(rows // chunk):
                y = cosine * co[i : i + 1] - sine * so[i : i + 1]
                high = y.astype(BF16)
                place = (pl.ds(i * chunk, chunk), pl.ds(pl.multiple_of(c * LANES, LANES), LANES))
                outs[2 * parity][place] = high
                outs[2 * parity + 1][place] = (y - high.astype(F32)).astype(BF16)
        return 0

    lax.fori_loop(0, width // LANES, column, 0)


def cosine_tables(fold, idx, cols):
    total = fold * cols
    side = total // 2
    return pl.pallas_call(
        functools.partial(table_kernel, total, cols, fold, 128),
        out_shape=[jax.ShapeDtypeStruct((side, side), BF16)] * 4,
        in_specs=smem(1),
        out_specs=vmem(4),
        compiler_params=params(),
        cost_estimate=pl.CostEstimate(flops=side * side * 60, bytes_accessed=side * side * 8, transcendentals=0),
        name="table",
    )(idx)


def weight_of(d):
    t = (1.0 - d) * (1.0 + d)
    return t * jnp.sqrt(t)


def lane_pick(x, index):
    return jnp.take_along_axis(x, index, axis=1)


def transform_kernel(fold, at, sizes, cuts, last, idx, *refs):
    take = iter(refs)
    xs = [next(take) for _ in range(fold)]
    tables = [next(take) for _ in range(4)]
    damp = [next(take) for _ in range(fold)]
    if last:
        earlier = next(take)
    outs = [[next(take) for _ in pieces] for pieces in cuts]
    if last:
        ends = [next(take) for _ in range(fold)]
    else:
        ends_all = next(take)
    parts = [next(take) for _ in range(2)]
    half = sizes[last]
    planes, cols = xs[1].shape[1:]
    lane = lax.broadcasted_iota(jnp.int32, (planes, LANES), 1)
    tiles = cols // LANES

    def fold_cell(j, _):
        for p in range(fold // 2):
            a, b = xs[p], xs[fold - 1 - p]
            for t in range(tiles):
                x = a[j + (at if p == 0 else 0), :, pl.ds(t * LANES, LANES)]
                y = b[j, :, pl.ds((tiles - 1 - t) * LANES, LANES)]
                y = lane_pick(y, LANES - 1 - lane)
                for parity in range(2):
                    v = x - y if parity else x + y
                    high = v.astype(BF16)
                    columns = pl.ds(p * cols + t * LANES, LANES)
                    place = pl.multiple_of(j * planes, planes)
                    parts[parity][pl.ds(place, planes), columns] = high
                    parts[parity][pl.ds(half * planes + place, planes), columns] = (v - high.astype(F32)).astype(BF16)
        return 0

    lax.fori_loop(0, half, fold_cell, 0)

    rows = half * planes
    modes = cols // 2
    wide = lax.broadcasted_iota(jnp.int32, (rows, LANES), 1)
    for r in range(fold):
        columns = pl.ds(r * modes, modes)
        sums = []
        for parity in range(2):
            dot = functools.partial(jnp.dot, preferred_element_type=F32)
            both = dot(parts[parity][...], tables[2 * parity][:, columns])
            rest = dot(parts[parity][:rows], tables[2 * parity + 1][:, columns])
            sums.append(both[:rows] + both[rows:] + rest)
        for t in range(tiles):
            source = slice((t // 2) * LANES, (t // 2 + 1) * LANES)
            index = wide // 2 + (t % 2) * (LANES // 2)
            even, odd = (lane_pick(s[:, source], index) for s in sums)
            tile = jnp.where(wide % 2 == 0, even, odd)
            tile = tile.reshape(half, planes, LANES)
            for out, (low, high) in zip(outs[r], cuts[r]):
                out[:, :, pl.ds(t * LANES, LANES)] = tile[low:high]

    for r in range(fold):
        for t in range(tiles):
            at_lanes = pl.ds(t * LANES, LANES)
            d = damp[r][:, at_lanes]
            w = weight_of(d)
            f = jnp.zeros_like(d)
            forward = []
            for out, (low, high) in zip(outs[r], cuts[r]):
                for j in range(high - low):
                    f = w * out[j, :, at_lanes] + d * f
                    forward.append(f)
            p = jnp.zeros_like(d)
            for j in reversed(range(half)):
                p = forward[j] + d * p
            if last:
                f0, p0 = earlier[0, r, :, at_lanes], earlier[1, r, :, at_lanes]
                f, p = merge((f, p), (f0, p0), idx[0] != 0, span(d, half), span(d, sizes[0]))
                ends[r][0, :, at_lanes] = f
                ends[r][1, :, at_lanes] = p
            else:
                ends_all[0, r, :, at_lanes] = f
                ends_all[1, r, :, at_lanes] = p


def transform(fold, idx, sub, cuts, last, xs, tables, extra):
    planes, cols = xs[0].shape[1:]
    sizes = chunks(sub)
    half = sizes[last]
    at = sizes[0] if last else 0
    side = tables[0].shape[0]
    shape = lambda *n: jax.ShapeDtypeStruct(n, F32)
    outs = [shape(high - low, planes, cols) for pieces in cuts for low, high in pieces]
    if last:
        outs += [shape(2, planes, cols)] * fold
    else:
        outs += [shape(2, fold, planes, cols)]
    rows = half * planes
    return pl.pallas_call(
        functools.partial(transform_kernel, fold, at, sizes, cuts, last),
        out_shape=outs,
        in_specs=smem(1) + vmem(len(xs) + 4 + len(extra)),
        out_specs=vmem(len(outs)),
        scratch_shapes=[pltpu.VMEM((2 * rows, side), BF16)] * 2,
        compiler_params=params(),
        cost_estimate=pl.CostEstimate(flops=12 * rows * side * side, bytes_accessed=8 * side * side, transcendentals=0),
        name="transform_b" if last else "transform_a",
    )(idx, *xs, *tables, *extra)


def span(d, cells):
    power, gain, block = None, None, (d, d)
    while cells:
        if cells % 2:
            if power is None:
                power, gain = block
            else:
                power, gain = power * block[0], gain + power * power * block[1]
        block = doubled(*block)
        cells //= 2
    return power, gain


def merge(mine, other, upper, span_mine, span_other):
    pick = lambda a, b: a if a is b else jnp.where(upper, a, b)
    f_low, f_high = jnp.where(upper, other[0], mine[0]), jnp.where(upper, mine[0], other[0])
    p_low, p_high = jnp.where(upper, other[1], mine[1]), jnp.where(upper, mine[1], other[1])
    high_power, high_gain = pick(span_mine[0], span_other[0]), pick(span_mine[1], span_other[1])
    low_power = pick(span_other[0], span_mine[0])
    return f_high + high_power * f_low, p_low + low_power * (p_high + high_gain * f_low)


def doubled(power, gain):
    return power * power, gain * (1.0 + power * power)


def stages(fold, count):
    bits = [1 << k for k in range(count.bit_length() - 1)]
    groups = [[1 << k for k in range(fold.bit_length() - 1)]]
    return groups + [bits[k : k + 2] for k in range(0, len(bits), 2)]


def peers(bits):
    offsets = [0]
    for bit in bits:
        offsets += [o ^ bit for o in offsets]
    return offsets


def combine(groups, stage, d, sub, me, row, ends, entry):
    power, gain = span(d, sub)
    start, stop, turn = None, None, None
    for k, bits in enumerate(groups[: stage + 1]):
        position = row if k else me
        if k == 1:
            start, stop, turn = jnp.ones_like(d), jnp.ones_like(d), jnp.zeros_like(d)
            if entry is None:
                entry = (jnp.zeros_like(d), jnp.zeros_like(d))
        for bit in bits:
            upper = position & bit != 0
            if k:
                if k == stage:
                    mine, other = ends[0], ends[1]
                    below, above = entry
                    below = below + jnp.where(upper, start * other[0], 0.0)
                    above = above + jnp.where(upper, turn * other[0], stop * (other[1] + gain * mine[0]))
                    entry = (below, above)
                turn = jnp.where(upper, power * turn, turn + stop * gain * power)
                start = jnp.where(upper, power * start, start)
                stop = jnp.where(upper, stop, power * stop)
            if k == stage:
                ends = [merge(ends[i], ends[i + 1], upper, (power, gain), (power, gain)) for i in range(0, len(ends), 2)]
            power, gain = doubled(power, gain)
    return ends[0], entry


def combine_tiles(groups, stage, sub, idx, damping, ends, entry, put):
    for t in range(damping.shape[1] // LANES):
        at = pl.ds(t * LANES, LANES)
        pairs = [(e[0, :, at], e[1, :, at]) for e in ends]
        entered = None if entry is None else (entry[0, :, at], entry[1, :, at])
        put(at, *combine(groups, stage, damping[:, at], sub, idx[0], idx[1], pairs, entered))


def combine_kernel(groups, stage, sub, idx, damping, *refs):
    count = 1 << len(groups[stage])
    ends, rest = refs[:count], refs[count:]
    entry = rest[0] if stage > 1 else None
    outs = rest[-2:] if stage else rest[-1:]

    def put(at, union, entered):
        outs[0][0, :, at], outs[0][1, :, at] = union
        if stage:
            outs[1][0, :, at], outs[1][1, :, at] = entered

    combine_tiles(groups, stage, sub, idx, damping, ends, entry, put)


def combined(groups, stage, sub, idx, damping, ends, entry):
    pair = jax.ShapeDtypeStruct((2,) + damping.shape, F32)
    extra = [entry] if stage > 1 else []
    outs = [pair, pair] if stage else [pair]
    return pl.pallas_call(
        functools.partial(combine_kernel, groups, stage, sub),
        out_shape=outs,
        in_specs=smem(1) + vmem(1 + len(ends) + len(extra)),
        out_specs=vmem(len(outs)),
        compiler_params=params(),
        cost_estimate=pl.CostEstimate(flops=100 * damping.size, bytes_accessed=32 * damping.size, transcendentals=0),
    )(idx, damping, *ends, *extra)


def place(fold, cuts, me, sub):
    return [
        (chunk_start(me ^ r, h, sub) + low, high - low)
        for h in range(2)
        for r in range(fold)
        for low, high in cuts[h][r]
    ]


def gather_kernel(fold, cuts, chosen, idx, *refs):
    pieces, (gathered, out, sems) = refs[: len(chosen)], refs[len(chosen) :]
    places = place(fold, cuts, idx[0], gathered.shape[0] // fold)
    copies = []
    for n, k in enumerate(chosen):
        rows = pl.ds(*places[k])
        gathered[rows] = pieces[n][...]
        copies.append(pltpu.make_async_copy(gathered.at[rows], out.at[rows], sems.at[n]))
        copies[n].start()
    for copy in copies:
        copy.wait()


def gather(fold, cuts, idx, pieces, chosen, shape):
    return pl.pallas_call(
        functools.partial(gather_kernel, fold, cuts, chosen),
        out_shape=[jax.ShapeDtypeStruct(shape, F32)] * 2,
        in_specs=smem(1) + vmem(len(chosen)),
        out_specs=vmem(1) + hbm(1),
        scratch_shapes=[pltpu.SemaphoreType.DMA((len(chosen),))],
        compiler_params=params(),
        cost_estimate=pl.CostEstimate(flops=math.prod(shape), bytes_accessed=8 * math.prod(shape), transcendentals=0),
        name="gather",
    )(idx, *[pieces[k] for k in chosen])


def solve_kernel(fold, groups, cuts, chosen, idx, damping, *refs):
    stage = len(groups) - 1
    count = 1 << len(groups[stage])
    ends, rest = refs[:count], refs[count:]
    if stage > 1:
        entry, rest = rest[0], rest[1:]
    else:
        entry = None
    pieces, rest = rest[: len(chosen)], rest[len(chosen) :]
    _, _, coefficients, coefficients_out, pressure_out, pressure, entered, c_sems, p_sems = rest
    cells = coefficients.shape[0]
    sub = cells // fold
    half = sub // 2
    places = place(fold, cuts, idx[0], sub)
    copies = []
    for n, k in enumerate(chosen):
        rows = pl.ds(*places[k])
        coefficients[rows] = pieces[n][...]
        copies.append(pltpu.make_async_copy(coefficients.at[rows], coefficients_out.at[rows], c_sems.at[n]))
        copies[n].start()

    def put(at, union, entry):
        entered[0, :, at], entered[1, :, at] = entry

    combine_tiles(groups, stage, sub, idx, damping, ends, entry, put)
    d = damping[...]
    w = weight_of(d)

    def forward(i, f):
        f = w * coefficients[i] + d * f
        pressure[i] = f
        return f

    lax.fori_loop(0, cells, forward, entered[0], unroll=4)

    p = entered[1]
    for block in reversed(range(2 * fold)):

        def backward(i, p, block=block):
            at = (block + 1) * half - 1 - i
            p = pressure[at] + d * p
            pressure[at] = p
            return p

        p = lax.fori_loop(0, half, backward, p, unroll=4)
        rows = pl.ds(block * half, half)
        copies.append(pltpu.make_async_copy(pressure.at[rows], pressure_out.at[rows], p_sems.at[block]))
        copies[-1].start()
    for copy in copies:
        copy.wait()


def solve(fold, groups, cuts, idx, damping, ends, entry, pieces, chosen, gathered, partly):
    extra = [entry] if len(groups) > 2 else []
    operands = [idx, damping, *ends, *extra, *[pieces[k] for k in chosen], gathered, partly]
    shape = jax.ShapeDtypeStruct(gathered.shape, F32)
    return pl.pallas_call(
        functools.partial(solve_kernel, fold, groups, cuts, chosen),
        out_shape=[shape] * 3,
        in_specs=smem(1) + vmem(len(operands) - 2) + hbm(1),
        out_specs=vmem(1) + hbm(2),
        scratch_shapes=[
            pltpu.VMEM(gathered.shape, F32),
            pltpu.VMEM((2,) + damping.shape, F32),
            pltpu.SemaphoreType.DMA((len(chosen),)),
            pltpu.SemaphoreType.DMA((2 * fold,)),
        ],
        input_output_aliases={len(operands) - 2: 0, len(operands) - 1: 1},
        compiler_params=params(),
        cost_estimate=pl.CostEstimate(flops=5 * gathered.size, bytes_accessed=12 * gathered.size, transcendentals=0),
        name="solve",
    )(*operands)[1:]


def body(velocity_u, wall_strain, damping):
    cells, planes, cols = velocity_u.shape
    fold = lax.axis_size("gy")
    sub = cells // fold
    me, row = lax.axis_index("gy"), lax.axis_index("gx")
    idx = jnp.stack([me, row]).astype(jnp.int32)
    order = list(range(fold - 1, 0, -1))
    *sends, near, far, u, wall = lead(fold, idx, velocity_u, wall_strain)
    got = {(r, 0): partner(sends[r - 1], "gy", r) for r in order}
    near, far = exchange_edges(near, far)
    damp = {0: damping}
    bit = fold // 2
    while bit:
        damp |= {r ^ bit: partner(x, "gy", bit) for r, x in damp.items()}
        bit //= 2
    damp = [damp[r] for r in range(fold)]
    second, own, *sends = stencil(fold, idx, u, wall, near, far)
    for r in order:
        got[r, 1] = partner(sends[r - 1], "gy", r)
    tables = cosine_tables(fold, idx, cols)
    cuts = pieces_of(fold, sub)
    first = transform(fold, idx, sub, cuts[0], 0, [own] + [got[r, 0] for r in range(1, fold)], tables, damp)
    extra = [*damp, first[-1]]
    rest = transform(fold, idx, sub, cuts[1], 1, [own] + [got[r, 1] for r in range(1, fold)], tables, extra)
    ends_b = rest[-fold:]
    pieces = []
    for h, outs in enumerate((first, rest)):
        outs = iter(outs)
        for r in range(fold):
            for k in range(len(cuts[h][r])):
                out = next(outs)
                pieces.append(out if r == 0 else partner(out, "gy", r))
    groups = stages(fold, lax.axis_size("gx"))
    ends = [ends_b[r] if r == 0 else partner(ends_b[r], "gy", r) for r in peers(groups[0])]
    entry = None
    for stage in range(1, len(groups)):
        mine, *entries = combined(groups, stage - 1, sub, idx, damping, ends, entry)
        entry = entries[0] if entries else None
        ends = [mine] + [partner(mine, "gx", o) for o in peers(groups[stage])[1:]]
    late, k = [], 0
    for h in range(2):
        for r in range(fold):
            late += [k + n for n in range(len(cuts[h][r])) if h == 1 and r > 1]
            k += len(cuts[h][r])
    early = [n for n in range(k) if n not in late]
    gathered, partly = gather(fold, cuts, idx, pieces, early, (cells, planes, cols))
    coefficients, pressure = solve(fold, groups, cuts, idx, damping, ends, entry, pieces, late, gathered, partly)
    return second, coefficients, pressure


def pieces_of(fold, sub):
    first, later = chunks(sub)
    cut = first // 2
    whole = [[(0, first)] for _ in range(fold)]
    whole[fold - 1] = [(0, cut), (cut, first)]
    return whole, [[(0, later)] for _ in range(fold)]


def solution(mesh):
    return jax.shard_map(
        body,
        mesh=mesh,
        in_specs=(P("gx", None, "gy"), P("gx", None, "gy"), P(None, "gy")),
        out_specs=(P("gx", None, "gy"), P("gx", None, "gy"), P("gx", None, "gy")),
        check_vma=False,
    )
```

```python
import functools
import math

import jax
import jax.numpy as jnp
from jax import lax
from jax.experimental import pallas as pl
from jax.experimental.pallas import tpu as pltpu
from jax.sharding import PartitionSpec as P


LANES = 128
REACH = 3
F32 = jnp.float32
BF16 = jnp.bfloat16
MIB = 1024 * 1024
FIRST_LIMIT = 52 * MIB


def params(limit=16 * MIB):
    return pltpu.CompilerParams(vmem_limit_bytes=limit)


def vmem(count):
    return [pl.BlockSpec(memory_space=pltpu.VMEM)] * count


def at_device(kernel, *static):
    return lambda *refs: kernel(*static, (lax.axis_index("gy"), lax.axis_index("gx")), *refs)


def hbm(count):
    return [pl.BlockSpec(memory_space=pltpu.HBM)] * count


def partner(x, axis, bit):
    count = lax.axis_size(axis)
    return lax.ppermute(x, axis, [(i, i ^ bit) for i in range(count)])


def chunks(sub):
    later = max(5 * sub // 16, REACH)
    return sub - later, later


def chunk_start(block, h, sub):
    first, later = chunks(sub)
    return block * sub + (jnp.where(block == 0, later, 0) if h == 0 else jnp.where(block == 0, 0, first))


def derivatives(cell, at):
    c = [cell(at + k) for k in range(2 * REACH + 1)]
    first = 0.75 * (c[4] - c[2]) - 3.0 / 20.0 * (c[5] - c[1]) + 1.0 / 60.0 * (c[6] - c[0])
    second = (
        1.5 * (c[4] + c[2])
        - 3.0 / 20.0 * (c[5] + c[1])
        + 1.0 / 90.0 * (c[6] + c[0])
        - 49.0 / 18.0 * c[3]
    )
    return first, second


def first_kernel(fold, idx, u_in, wall_in, send, ubuf, wbuf, sems):
    size = send.shape[0]
    start = chunk_start(idx[0] ^ (fold - 1), 0, u_in.shape[0] // fold)
    u_copy = pltpu.make_async_copy(u_in.at[pl.ds(start - REACH, size + 2 * REACH)], ubuf, sems.at[0])
    w_copy = pltpu.make_async_copy(wall_in.at[pl.ds(start, size)], wbuf, sems.at[1])
    u_copy.start()
    w_copy.start()
    u_copy.wait()
    w_copy.wait()

    def step(j, _):
        first, _ = derivatives(lambda k: ubuf[k], j)
        send[j] = first + wbuf[j]
        return 0

    lax.fori_loop(0, size, step, 0, unroll=2)


def first_cells(fold, u, wall):
    cells, planes, cols = u.shape
    size = chunks(cells // fold)[0]
    return pl.pallas_call(
        at_device(first_kernel, fold),
        out_shape=jax.ShapeDtypeStruct((size, planes, cols), F32),
        in_specs=hbm(2),
        out_specs=vmem(1)[0],
        scratch_shapes=[
            pltpu.VMEM((size + 2 * REACH, planes, cols), F32),
            pltpu.VMEM((size, planes, cols), F32),
            pltpu.SemaphoreType.DMA((2,)),
        ],
        compiler_params=params(FIRST_LIMIT),
        cost_estimate=pl.CostEstimate(flops=size * planes * cols * 10, bytes_accessed=size * planes * cols * 12, transcendentals=0),
        name="first",
    )(u, wall)


def lead_kernel(fold, idx, u, wall, *refs):
    sends, (near, far) = refs[: fold - 2], refs[fold - 2 :]
    cells = u.shape[0]
    sub = cells // fold
    me, row = idx
    even = row % 2 == 0
    near[...] = u[pl.ds(jnp.where(even, cells - REACH, 0), REACH)]
    far[...] = u[pl.ds(jnp.where(even, 0, cells - REACH), REACH)]
    for r in range(fold - 2, 0, -1):
        start = chunk_start(me ^ r, 0, sub)

        def step(j, _, r=r, start=start):
            first, _ = derivatives(lambda k: u[k], start - REACH + j)
            sends[r - 1][j] = first + wall[start + j]
            return 0

        lax.fori_loop(0, chunks(sub)[0], step, 0, unroll=2)


def lead(fold, u, wall):
    cells, planes, cols = u.shape
    shape = lambda n: jax.ShapeDtypeStruct((n, planes, cols), F32)
    outs = [shape(chunks(cells // fold)[0])] * (fold - 2) + [shape(REACH)] * 2
    return pl.pallas_call(
        at_device(lead_kernel, fold),
        out_shape=outs,
        in_specs=vmem(2),
        out_specs=vmem(len(outs)),
        compiler_params=params(),
        cost_estimate=pl.CostEstimate(flops=cells * planes * cols * 6, bytes_accessed=cells * planes * cols * 6, transcendentals=0),
        name="lead",
    )(u, wall)


def stencil_kernel(fold, idx, u, wall, near, far, second_out, *refs):
    own, sends, (pad, second, out_sems) = refs[0], refs[1:fold], refs[fold:]
    cells = u.shape[0]
    sub = cells // fold
    sizes = chunks(sub)
    me = idx[0]
    even = idx[1] % 2 == 0
    pad[pl.ds(REACH, cells)] = u[...]
    pad[pl.ds(0, REACH)] = jnp.where(even, far[...], near[...])
    pad[pl.ds(REACH + cells, REACH)] = jnp.where(even, near[...], far[...])
    out_copies = []
    for r in range(fold - 1, -1, -1):
        block = me ^ r
        for h in (1, 0):
            start = chunk_start(block, h, sub)

            def step(j, _, r=r, h=h, start=start):
                first, second[start + j] = derivatives(lambda k: pad[k], start + j)
                if r == 0:
                    own[h * sizes[0] + j] = first + wall[start + j]
                elif h == 1:
                    sends[r - 1][j] = first + wall[start + j]
                return 0

            lax.fori_loop(0, sizes[h], step, 0, unroll=2)
        rows = pl.ds(block * sub, sub)
        copy = pltpu.make_async_copy(second.at[rows], second_out.at[rows], out_sems.at[r])
        copy.start()
        out_copies.append(copy)
    for copy in out_copies:
        copy.wait()


def stencil(fold, u, wall, near, far):
    cells, planes, cols = u.shape
    sub = cells // fold
    later = chunks(sub)[1]
    shape = lambda n: jax.ShapeDtypeStruct((n, planes, cols), F32)
    outs = [shape(cells), shape(sub)] + [shape(later)] * (fold - 1)
    return pl.pallas_call(
        at_device(stencil_kernel, fold),
        out_shape=outs,
        in_specs=vmem(4),
        out_specs=hbm(1) + vmem(len(outs) - 1),
        scratch_shapes=[
            pltpu.VMEM((cells + 2 * REACH, planes, cols), F32),
            pltpu.VMEM((cells, planes, cols), F32),
            pltpu.SemaphoreType.DMA((fold,)),
        ],
        compiler_params=params(),
        cost_estimate=pl.CostEstimate(flops=cells * planes * cols * 20, bytes_accessed=cells * planes * cols * 16, transcendentals=0),
        name="stencil",
    )(u, wall, near, far)


def exchange_edges(near, far):
    count = lax.axis_size("gx")
    inner = [(i, i + 1) for i in range(1, count - 1, 2)]
    far = lax.ppermute(far, "gx", inner + [(b, a) for a, b in inner])
    return partner(near, "gx", 1), far


def half_turn(phase, total):
    phase = phase - jnp.floor(phase * (1.0 / (4 * total))) * (4.0 * total)
    x = (jnp.abs(phase - 2.0 * total) - total) * (math.pi / (2.0 * total))
    s = x * x
    y = -1.0 / 39916800.0
    for coefficient in (1.0 / 362880.0, -1.0 / 5040.0, 1.0 / 120.0, -1.0 / 6.0, 1.0):
        y = y * s + coefficient
    return y * x


def table_kernel(total, cols, fold, chunk, idx, *outs):
    rows, width = outs[0].shape
    me = idx[0]
    modes = width // fold
    group = 8
    whole = lambda *shape: lambda axis: lax.broadcasted_iota(jnp.int32, shape, axis)
    base, inner, outer = whole(group, LANES), whole(chunk // group, LANES), whole(rows // chunk, LANES)
    at = outer(0) * chunk
    block = at // cols
    shifts = ((me ^ block) * cols + (at - block * cols)).astype(F32) * 2.0
    steps = (inner(0) * (2 * group)).astype(F32)
    sample = base(0).astype(F32) * 2.0 + 1.0

    def both(phase):
        return half_turn(phase, total), half_turn(phase - total, total)

    def column(c, _):
        r = c * LANES // modes
        first = (me ^ r) * modes + (c * LANES - r * modes)
        for parity in range(2):
            mode = lambda iota: (first + iota(1)).astype(F32) * 2.0 + parity
            c0, s0 = (v * math.sqrt(2.0 / total) for v in both(sample * mode(base)))
            ci, si = both(steps * mode(inner))
            co, so = both(shifts * mode(outer))
            cosine = jnp.concatenate([c0 * ci[i : i + 1] - s0 * si[i : i + 1] for i in range(chunk // group)])
            sine = jnp.concatenate([s0 * ci[i : i + 1] + c0 * si[i : i + 1] for i in range(chunk // group)])
            for i in range(rows // chunk):
                y = cosine * co[i : i + 1] - sine * so[i : i + 1]
                high = y.astype(BF16)
                place = (pl.ds(i * chunk, chunk), pl.ds(pl.multiple_of(c * LANES, LANES), LANES))
                outs[2 * parity][place] = high
                outs[2 * parity + 1][place] = (y - high.astype(F32)).astype(BF16)
        return 0

    lax.fori_loop(0, width // LANES, column, 0)


def cosine_tables(fold, cols):
    total = fold * cols
    side = total // 2
    return pl.pallas_call(
        at_device(table_kernel, total, cols, fold, 128),
        out_shape=[jax.ShapeDtypeStruct((side, side), BF16)] * 4,
        out_specs=vmem(4),
        compiler_params=params(),
        cost_estimate=pl.CostEstimate(flops=side * side * 60, bytes_accessed=side * side * 8, transcendentals=0),
        name="table",
    )()


def weight_of(d):
    t = (1.0 - d) * (1.0 + d)
    return t * jnp.sqrt(t)


def lane_pick(x, index):
    return jnp.take_along_axis(x, index, axis=1)


def transform_kernel(fold, at, sizes, cuts, last, idx, *refs):
    take = iter(refs)
    xs = [next(take) for _ in range(fold)]
    tables = [next(take) for _ in range(4)]
    damp = [next(take) for _ in range(fold)]
    if last:
        earlier = next(take)
    outs = [[next(take) for _ in pieces] for pieces in cuts]
    if last:
        ends = [next(take) for _ in range(fold)]
    else:
        ends_all = next(take)
    parts = [next(take) for _ in range(2)]
    half = sizes[last]
    planes, cols = xs[1].shape[1:]
    lane = lax.broadcasted_iota(jnp.int32, (planes, LANES), 1)
    tiles = cols // LANES

    def fold_cell(j, _):
        for p in range(fold // 2):
            a, b = xs[p], xs[fold - 1 - p]
            for t in range(tiles):
                x = a[j + (at if p == 0 else 0), :, pl.ds(t * LANES, LANES)]
                y = b[j, :, pl.ds((tiles - 1 - t) * LANES, LANES)]
                y = lane_pick(y, LANES - 1 - lane)
                for parity in range(2):
                    v = x - y if parity else x + y
                    high = v.astype(BF16)
                    columns = pl.ds(p * cols + t * LANES, LANES)
                    place = pl.multiple_of(j * planes, planes)
                    parts[parity][pl.ds(place, planes), columns] = high
                    parts[parity][pl.ds(half * planes + place, planes), columns] = (v - high.astype(F32)).astype(BF16)
        return 0

    lax.fori_loop(0, half, fold_cell, 0)

    rows = half * planes
    modes = cols // 2
    wide = lax.broadcasted_iota(jnp.int32, (rows, LANES), 1)
    for r in range(fold):
        columns = pl.ds(r * modes, modes)
        sums = []
        for parity in range(2):
            dot = functools.partial(jnp.dot, preferred_element_type=F32)
            both = dot(parts[parity][...], tables[2 * parity][:, columns])
            rest = dot(parts[parity][:rows], tables[2 * parity + 1][:, columns])
            sums.append(both[:rows] + both[rows:] + rest)
        for t in range(tiles):
            source = slice((t // 2) * LANES, (t // 2 + 1) * LANES)
            index = wide // 2 + (t % 2) * (LANES // 2)
            even, odd = (lane_pick(s[:, source], index) for s in sums)
            tile = jnp.where(wide % 2 == 0, even, odd)
            tile = tile.reshape(half, planes, LANES)
            for out, (low, high) in zip(outs[r], cuts[r]):
                out[:, :, pl.ds(t * LANES, LANES)] = tile[low:high]

    for r in range(fold):
        for t in range(tiles):
            at_lanes = pl.ds(t * LANES, LANES)
            d = damp[r][:, at_lanes]
            w = weight_of(d)
            f = jnp.zeros_like(d)
            forward = []
            for out, (low, high) in zip(outs[r], cuts[r]):
                for j in range(high - low):
                    f = w * out[j, :, at_lanes] + d * f
                    forward.append(f)
            p = jnp.zeros_like(d)
            for j in reversed(range(half)):
                p = forward[j] + d * p
            if last:
                f0, p0 = earlier[0, r, :, at_lanes], earlier[1, r, :, at_lanes]
                f, p = merge((f, p), (f0, p0), idx[0] != 0, span(d, half), span(d, sizes[0]))
                ends[r][0, :, at_lanes] = f
                ends[r][1, :, at_lanes] = p
            else:
                ends_all[0, r, :, at_lanes] = f
                ends_all[1, r, :, at_lanes] = p


def transform(fold, sub, cuts, last, xs, tables, extra):
    planes, cols = xs[0].shape[1:]
    sizes = chunks(sub)
    half = sizes[last]
    at = sizes[0] if last else 0
    side = tables[0].shape[0]
    shape = lambda *n: jax.ShapeDtypeStruct(n, F32)
    outs = [shape(high - low, planes, cols) for pieces in cuts for low, high in pieces]
    if last:
        outs += [shape(2, planes, cols)] * fold
    else:
        outs += [shape(2, fold, planes, cols)]
    rows = half * planes
    return pl.pallas_call(
        at_device(transform_kernel, fold, at, sizes, cuts, last),
        out_shape=outs,
        in_specs=vmem(len(xs) + 4 + len(extra)),
        out_specs=vmem(len(outs)),
        scratch_shapes=[pltpu.VMEM((2 * rows, side), BF16)] * 2,
        compiler_params=params(),
        cost_estimate=pl.CostEstimate(flops=12 * rows * side * side, bytes_accessed=8 * side * side, transcendentals=0),
        name="transform_b" if last else "transform_a",
    )(*xs, *tables, *extra)


def span(d, cells):
    power, gain, block = None, None, (d, d)
    while cells:
        if cells % 2:
            if power is None:
                power, gain = block
            else:
                power, gain = power * block[0], gain + power * power * block[1]
        block = doubled(*block)
        cells //= 2
    return power, gain


def merge(mine, other, upper, span_mine, span_other):
    pick = lambda a, b: a if a is b else jnp.where(upper, a, b)
    f_low, f_high = jnp.where(upper, other[0], mine[0]), jnp.where(upper, mine[0], other[0])
    p_low, p_high = jnp.where(upper, other[1], mine[1]), jnp.where(upper, mine[1], other[1])
    high_power, high_gain = pick(span_mine[0], span_other[0]), pick(span_mine[1], span_other[1])
    low_power = pick(span_other[0], span_mine[0])
    return f_high + high_power * f_low, p_low + low_power * (p_high + high_gain * f_low)


def doubled(power, gain):
    return power * power, gain * (1.0 + power * power)


def stages(fold, count):
    bits = [1 << k for k in range(count.bit_length() - 1)]
    groups = [[1 << k for k in range(fold.bit_length() - 1)]]
    return groups + [bits[k : k + 2] for k in range(0, len(bits), 2)]


def peers(bits):
    offsets = [0]
    for bit in bits:
        offsets += [o ^ bit for o in offsets]
    return offsets


def combine(groups, stage, d, sub, me, row, ends, entry):
    power, gain = span(d, sub)
    start, stop, turn = None, None, None
    for k, bits in enumerate(groups[: stage + 1]):
        position = row if k else me
        if k == 1:
            start, stop, turn = jnp.ones_like(d), jnp.ones_like(d), jnp.zeros_like(d)
            if entry is None:
                entry = (jnp.zeros_like(d), jnp.zeros_like(d))
        for bit in bits:
            upper = position & bit != 0
            if k:
                if k == stage:
                    mine, other = ends[0], ends[1]
                    below, above = entry
                    below = below + jnp.where(upper, start * other[0], 0.0)
                    above = above + jnp.where(upper, turn * other[0], stop * (other[1] + gain * mine[0]))
                    entry = (below, above)
                turn = jnp.where(upper, power * turn, turn + stop * gain * power)
                start = jnp.where(upper, power * start, start)
                stop = jnp.where(upper, stop, power * stop)
            if k == stage:
                ends = [merge(ends[i], ends[i + 1], upper, (power, gain), (power, gain)) for i in range(0, len(ends), 2)]
            power, gain = doubled(power, gain)
    return ends[0], entry


def combine_tiles(groups, stage, sub, idx, damping, ends, entry, put):
    for t in range(damping.shape[1] // LANES):
        at = pl.ds(t * LANES, LANES)
        pairs = [(e[0, :, at], e[1, :, at]) for e in ends]
        entered = None if entry is None else (entry[0, :, at], entry[1, :, at])
        put(at, *combine(groups, stage, damping[:, at], sub, idx[0], idx[1], pairs, entered))


def combine_kernel(groups, stage, sub, idx, damping, *refs):
    count = 1 << len(groups[stage])
    ends, rest = refs[:count], refs[count:]
    entry = rest[0] if stage > 1 else None
    outs = rest[-2:] if stage else rest[-1:]

    def put(at, union, entered):
        outs[0][0, :, at], outs[0][1, :, at] = union
        if stage:
            outs[1][0, :, at], outs[1][1, :, at] = entered

    combine_tiles(groups, stage, sub, idx, damping, ends, entry, put)


def combined(groups, stage, sub, damping, ends, entry):
    pair = jax.ShapeDtypeStruct((2,) + damping.shape, F32)
    extra = [entry] if stage > 1 else []
    outs = [pair, pair] if stage else [pair]
    return pl.pallas_call(
        at_device(combine_kernel, groups, stage, sub),
        out_shape=outs,
        in_specs=vmem(1 + len(ends) + len(extra)),
        out_specs=vmem(len(outs)),
        compiler_params=params(),
        cost_estimate=pl.CostEstimate(flops=100 * damping.size, bytes_accessed=32 * damping.size, transcendentals=0),
    )(damping, *ends, *extra)


def place(fold, cuts, me, sub):
    return [
        (chunk_start(me ^ r, h, sub) + low, high - low)
        for h in range(2)
        for r in range(fold)
        for low, high in cuts[h][r]
    ]


def gather_kernel(fold, cuts, chosen, idx, *refs):
    pieces, (gathered, out, sems) = refs[: len(chosen)], refs[len(chosen) :]
    places = place(fold, cuts, idx[0], gathered.shape[0] // fold)
    copies = []
    for n, k in enumerate(chosen):
        rows = pl.ds(*places[k])
        gathered[rows] = pieces[n][...]
        copies.append(pltpu.make_async_copy(gathered.at[rows], out.at[rows], sems.at[n]))
        copies[n].start()
    for copy in copies:
        copy.wait()


def gather(fold, cuts, pieces, chosen, shape):
    return pl.pallas_call(
        at_device(gather_kernel, fold, cuts, chosen),
        out_shape=[jax.ShapeDtypeStruct(shape, F32)] * 2,
        in_specs=vmem(len(chosen)),
        out_specs=vmem(1) + hbm(1),
        scratch_shapes=[pltpu.SemaphoreType.DMA((len(chosen),))],
        compiler_params=params(),
        cost_estimate=pl.CostEstimate(flops=math.prod(shape), bytes_accessed=8 * math.prod(shape), transcendentals=0),
        name="gather",
    )(*[pieces[k] for k in chosen])


def solve_kernel(fold, groups, cuts, chosen, idx, damping, *refs):
    stage = len(groups) - 1
    count = 1 << len(groups[stage])
    ends, rest = refs[:count], refs[count:]
    if stage > 1:
        entry, rest = rest[0], rest[1:]
    else:
        entry = None
    pieces, rest = rest[: len(chosen)], rest[len(chosen) :]
    _, _, coefficients, coefficients_out, pressure_out, pressure, entered, c_sems, p_sems = rest
    cells = coefficients.shape[0]
    sub = cells // fold
    half = sub // 2
    places = place(fold, cuts, idx[0], sub)
    copies = []
    for n, k in enumerate(chosen):
        rows = pl.ds(*places[k])
        coefficients[rows] = pieces[n][...]
        copies.append(pltpu.make_async_copy(coefficients.at[rows], coefficients_out.at[rows], c_sems.at[n]))
        copies[n].start()

    def put(at, union, entry):
        entered[0, :, at], entered[1, :, at] = entry

    combine_tiles(groups, stage, sub, idx, damping, ends, entry, put)
    d = damping[...]
    w = weight_of(d)

    def forward(i, carry):
        f, now = carry
        following = coefficients[jnp.minimum(i + 1, cells - 1)]
        f = w * now + d * f
        pressure[i] = f
        return f, following

    lax.fori_loop(0, cells, forward, (entered[0], coefficients[0]), unroll=4)

    p = entered[1]
    for block in reversed(range(2 * fold)):

        def backward(i, p, block=block):
            at = (block + 1) * half - 1 - i
            p = pressure[at] + d * p
            pressure[at] = p
            return p

        p = lax.fori_loop(0, half, backward, p, unroll=4)
        rows = pl.ds(block * half, half)
        copies.append(pltpu.make_async_copy(pressure.at[rows], pressure_out.at[rows], p_sems.at[block]))
        copies[-1].start()
    for copy in copies:
        copy.wait()


def solve(fold, groups, cuts, damping, ends, entry, pieces, chosen, gathered, partly):
    extra = [entry] if len(groups) > 2 else []
    operands = [damping, *ends, *extra, *[pieces[k] for k in chosen], gathered, partly]
    shape = jax.ShapeDtypeStruct(gathered.shape, F32)
    return pl.pallas_call(
        at_device(solve_kernel, fold, groups, cuts, chosen),
        out_shape=[shape] * 3,
        in_specs=vmem(len(operands) - 1) + hbm(1),
        out_specs=vmem(1) + hbm(2),
        scratch_shapes=[
            pltpu.VMEM(gathered.shape, F32),
            pltpu.VMEM((2,) + damping.shape, F32),
            pltpu.SemaphoreType.DMA((len(chosen),)),
            pltpu.SemaphoreType.DMA((2 * fold,)),
        ],
        input_output_aliases={len(operands) - 2: 0, len(operands) - 1: 1},
        compiler_params=params(),
        cost_estimate=pl.CostEstimate(flops=5 * gathered.size, bytes_accessed=12 * gathered.size, transcendentals=0),
        name="solve",
    )(*operands)[1:]


def body(velocity_u, wall_strain, damping):
    cells, planes, cols = velocity_u.shape
    fold = lax.axis_size("gy")
    sub = cells // fold
    order = list(range(fold - 1, 0, -1))
    first_send = first_cells(fold, velocity_u, wall_strain)
    *sends, near, far = lead(fold, velocity_u, wall_strain)
    sends.append(first_send)
    got = {(r, 0): partner(sends[r - 1], "gy", r) for r in order}
    near, far = exchange_edges(near, far)
    damp = {0: damping}
    bit = fold // 2
    while bit:
        damp |= {r ^ bit: partner(x, "gy", bit) for r, x in damp.items()}
        bit //= 2
    damp = [damp[r] for r in range(fold)]
    second, own, *sends = stencil(fold, velocity_u, wall_strain, near, far)
    for r in order:
        got[r, 1] = partner(sends[r - 1], "gy", r)
    tables = cosine_tables(fold, cols)
    cuts = pieces_of(fold, sub)
    first = transform(fold, sub, cuts[0], 0, [own] + [got[r, 0] for r in range(1, fold)], tables, damp)
    extra = [*damp, first[-1]]
    rest = transform(fold, sub, cuts[1], 1, [own] + [got[r, 1] for r in range(1, fold)], tables, extra)
    ends_b = rest[-fold:]
    pieces = []
    for h, outs in enumerate((first, rest)):
        outs = iter(outs)
        for r in range(fold):
            for k in range(len(cuts[h][r])):
                out = next(outs)
                pieces.append(out if r == 0 else partner(out, "gy", r))
    groups = stages(fold, lax.axis_size("gx"))
    ends = [ends_b[r] if r == 0 else partner(ends_b[r], "gy", r) for r in peers(groups[0])]
    entry = None
    for stage in range(1, len(groups)):
        mine, *entries = combined(groups, stage - 1, sub, damping, ends, entry)
        entry = entries[0] if entries else None
        ends = [mine] + [partner(mine, "gx", o) for o in peers(groups[stage])[1:]]
    late, k = [], 0
    for h in range(2):
        for r in range(fold):
            late += [k + n for n in range(len(cuts[h][r])) if h == 1 and r > 1]
            k += len(cuts[h][r])
    early = [n for n in range(k) if n not in late]
    gathered, partly = gather(fold, cuts, pieces, early, (cells, planes, cols))
    coefficients, pressure = solve(fold, groups, cuts, damping, ends, entry, pieces, late, gathered, partly)
    return second, coefficients, pressure


def pieces_of(fold, sub):
    first, later = chunks(sub)
    cut = first // 2
    whole = [[(0, first)] for _ in range(fold)]
    whole[fold - 1] = [(0, cut), (cut, first)]
    return whole, [[(0, later)] for _ in range(fold)]


def solution(mesh):
    return jax.shard_map(
        body,
        mesh=mesh,
        in_specs=(P("gx", None, "gy"), P("gx", None, "gy"), P(None, "gy")),
        out_specs=(P("gx", None, "gy"), P("gx", None, "gy"), P("gx", None, "gy")),
        check_vma=False,
    )
```

```python
import functools
import math

import jax
import jax.numpy as jnp
from jax import lax
from jax.experimental import pallas as pl
from jax.experimental.pallas import tpu as pltpu
from jax.sharding import PartitionSpec as P


LANES = 128
REACH = 3
F32 = jnp.float32
BF16 = jnp.bfloat16
MIB = 1024 * 1024
FIRST_LIMIT = 52 * MIB


def params(limit=16 * MIB):
    return pltpu.CompilerParams(vmem_limit_bytes=limit)


def vmem(count):
    return [pl.BlockSpec(memory_space=pltpu.VMEM)] * count


def at_device(kernel, *static):
    return lambda *refs: kernel(*static, (lax.axis_index("gy"), lax.axis_index("gx")), *refs)


def hbm(count):
    return [pl.BlockSpec(memory_space=pltpu.HBM)] * count


def partner(x, axis, bit):
    count = lax.axis_size(axis)
    return lax.ppermute(x, axis, [(i, i ^ bit) for i in range(count)])


def chunks(sub):
    later = max(5 * sub // 16, REACH)
    return sub - later, later


def chunk_start(block, h, sub):
    first, later = chunks(sub)
    return block * sub + (jnp.where(block == 0, later, 0) if h == 0 else jnp.where(block == 0, 0, first))


def derivatives(cell, at):
    c = [cell(at + k) for k in range(2 * REACH + 1)]
    first = 0.75 * (c[4] - c[2]) - 3.0 / 20.0 * (c[5] - c[1]) + 1.0 / 60.0 * (c[6] - c[0])
    second = (
        1.5 * (c[4] + c[2])
        - 3.0 / 20.0 * (c[5] + c[1])
        + 1.0 / 90.0 * (c[6] + c[0])
        - 49.0 / 18.0 * c[3]
    )
    return first, second


def first_kernel(fold, idx, u_in, wall_in, send, ubuf, wbuf, sems):
    size = send.shape[0]
    start = chunk_start(idx[0] ^ (fold - 1), 0, u_in.shape[0] // fold)
    u_copy = pltpu.make_async_copy(u_in.at[pl.ds(start - REACH, size + 2 * REACH)], ubuf, sems.at[0])
    w_copy = pltpu.make_async_copy(wall_in.at[pl.ds(start, size)], wbuf, sems.at[1])
    u_copy.start()
    w_copy.start()
    u_copy.wait()
    w_copy.wait()

    def step(j, _):
        first, _ = derivatives(lambda k: ubuf[k], j)
        send[j] = first + wbuf[j]
        return 0

    lax.fori_loop(0, size, step, 0, unroll=2)


def first_cells(fold, u, wall):
    cells, planes, cols = u.shape
    size = chunks(cells // fold)[0]
    return pl.pallas_call(
        at_device(first_kernel, fold),
        out_shape=jax.ShapeDtypeStruct((size, planes, cols), F32),
        in_specs=hbm(2),
        out_specs=vmem(1)[0],
        scratch_shapes=[
            pltpu.VMEM((size + 2 * REACH, planes, cols), F32),
            pltpu.VMEM((size, planes, cols), F32),
            pltpu.SemaphoreType.DMA((2,)),
        ],
        compiler_params=params(FIRST_LIMIT),
        cost_estimate=pl.CostEstimate(flops=size * planes * cols * 10, bytes_accessed=size * planes * cols * 12, transcendentals=0),
        name="first",
    )(u, wall)


def lead_kernel(fold, idx, u, wall, *refs):
    sends, (near, far) = refs[: fold - 2], refs[fold - 2 :]
    cells = u.shape[0]
    sub = cells // fold
    me, row = idx
    even = row % 2 == 0
    near[...] = u[pl.ds(jnp.where(even, cells - REACH, 0), REACH)]
    far[...] = u[pl.ds(jnp.where(even, 0, cells - REACH), REACH)]
    for r in range(fold - 2, 0, -1):
        start = chunk_start(me ^ r, 0, sub)

        def step(j, _, r=r, start=start):
            first, _ = derivatives(lambda k: u[k], start - REACH + j)
            sends[r - 1][j] = first + wall[start + j]
            return 0

        lax.fori_loop(0, chunks(sub)[0], step, 0, unroll=2)


def lead(fold, u, wall):
    cells, planes, cols = u.shape
    shape = lambda n: jax.ShapeDtypeStruct((n, planes, cols), F32)
    outs = [shape(chunks(cells // fold)[0])] * (fold - 2) + [shape(REACH)] * 2
    return pl.pallas_call(
        at_device(lead_kernel, fold),
        out_shape=outs,
        in_specs=vmem(2),
        out_specs=vmem(len(outs)),
        compiler_params=params(),
        cost_estimate=pl.CostEstimate(flops=cells * planes * cols * 6, bytes_accessed=cells * planes * cols * 6, transcendentals=0),
        name="lead",
    )(u, wall)


def stencil_kernel(fold, idx, u, wall, near, far, second_out, *refs):
    own, sends, (pad, second, out_sems) = refs[0], refs[1:fold], refs[fold:]
    cells = u.shape[0]
    sub = cells // fold
    sizes = chunks(sub)
    me = idx[0]
    even = idx[1] % 2 == 0
    pad[pl.ds(REACH, cells)] = u[...]
    pad[pl.ds(0, REACH)] = jnp.where(even, far[...], near[...])
    pad[pl.ds(REACH + cells, REACH)] = jnp.where(even, near[...], far[...])
    out_copies = []
    for r in range(fold - 1, -1, -1):
        block = me ^ r
        for h in (1, 0):
            start = chunk_start(block, h, sub)

            def step(j, _, r=r, h=h, start=start):
                first, second[start + j] = derivatives(lambda k: pad[k], start + j)
                if r == 0:
                    own[h * sizes[0] + j] = first + wall[start + j]
                elif h == 1:
                    sends[r - 1][j] = first + wall[start + j]
                return 0

            lax.fori_loop(0, sizes[h], step, 0, unroll=2)
        rows = pl.ds(block * sub, sub)
        copy = pltpu.make_async_copy(second.at[rows], second_out.at[rows], out_sems.at[r])
        copy.start()
        out_copies.append(copy)
    for copy in out_copies:
        copy.wait()


def stencil(fold, u, wall, near, far):
    cells, planes, cols = u.shape
    sub = cells // fold
    later = chunks(sub)[1]
    shape = lambda n: jax.ShapeDtypeStruct((n, planes, cols), F32)
    outs = [shape(cells), shape(sub)] + [shape(later)] * (fold - 1)
    return pl.pallas_call(
        at_device(stencil_kernel, fold),
        out_shape=outs,
        in_specs=vmem(4),
        out_specs=hbm(1) + vmem(len(outs) - 1),
        scratch_shapes=[
            pltpu.VMEM((cells + 2 * REACH, planes, cols), F32),
            pltpu.VMEM((cells, planes, cols), F32),
            pltpu.SemaphoreType.DMA((fold,)),
        ],
        compiler_params=params(),
        cost_estimate=pl.CostEstimate(flops=cells * planes * cols * 20, bytes_accessed=cells * planes * cols * 16, transcendentals=0),
        name="stencil",
    )(u, wall, near, far)


def exchange_edges(near, far):
    count = lax.axis_size("gx")
    inner = [(i, i + 1) for i in range(1, count - 1, 2)]
    far = lax.ppermute(far, "gx", inner + [(b, a) for a, b in inner])
    return partner(near, "gx", 1), far


def half_turn(phase, total):
    phase = phase - jnp.floor(phase * (1.0 / (4 * total))) * (4.0 * total)
    x = (jnp.abs(phase - 2.0 * total) - total) * (math.pi / (2.0 * total))
    s = x * x
    y = -1.0 / 39916800.0
    for coefficient in (1.0 / 362880.0, -1.0 / 5040.0, 1.0 / 120.0, -1.0 / 6.0, 1.0):
        y = y * s + coefficient
    return y * x


def table_kernel(total, cols, fold, chunk, idx, *outs):
    rows, width = outs[0].shape
    me = idx[0]
    modes = width // fold
    group = 8
    whole = lambda *shape: lambda axis: lax.broadcasted_iota(jnp.int32, shape, axis)
    base, inner, outer = whole(group, LANES), whole(chunk // group, LANES), whole(rows // chunk, LANES)
    at = outer(0) * chunk
    block = at // cols
    shifts = ((me ^ block) * cols + (at - block * cols)).astype(F32) * 2.0
    steps = (inner(0) * (2 * group)).astype(F32)
    sample = base(0).astype(F32) * 2.0 + 1.0

    def both(phase):
        return half_turn(phase, total), half_turn(phase - total, total)

    def column(c, _):
        r = c * LANES // modes
        first = (me ^ r) * modes + (c * LANES - r * modes)
        for parity in range(2):
            mode = lambda iota: (first + iota(1)).astype(F32) * 2.0 + parity
            c0, s0 = (v * math.sqrt(2.0 / total) for v in both(sample * mode(base)))
            ci, si = both(steps * mode(inner))
            co, so = both(shifts * mode(outer))
            cosine = jnp.concatenate([c0 * ci[i : i + 1] - s0 * si[i : i + 1] for i in range(chunk // group)])
            sine = jnp.concatenate([s0 * ci[i : i + 1] + c0 * si[i : i + 1] for i in range(chunk // group)])
            for i in range(rows // chunk):
                y = cosine * co[i : i + 1] - sine * so[i : i + 1]
                high = y.astype(BF16)
                place = (pl.ds(i * chunk, chunk), pl.ds(pl.multiple_of(c * LANES, LANES), LANES))
                outs[2 * parity][place] = high
                outs[2 * parity + 1][place] = (y - high.astype(F32)).astype(BF16)
        return 0

    lax.fori_loop(0, width // LANES, column, 0)


def cosine_tables(fold, cols):
    total = fold * cols
    side = total // 2
    return pl.pallas_call(
        at_device(table_kernel, total, cols, fold, 128),
        out_shape=[jax.ShapeDtypeStruct((side, side), BF16)] * 4,
        out_specs=vmem(4),
        compiler_params=params(),
        cost_estimate=pl.CostEstimate(flops=side * side * 60, bytes_accessed=side * side * 8, transcendentals=0),
        name="table",
    )()


def weight_of(d):
    t = (1.0 - d) * (1.0 + d)
    return t * jnp.sqrt(t)


def lane_pick(x, index):
    return jnp.take_along_axis(x, index, axis=1)


def transform_kernel(fold, at, sizes, cuts, last, idx, *refs):
    take = iter(refs)
    xs = [next(take) for _ in range(fold)]
    tables = [next(take) for _ in range(4)]
    damp = [next(take) for _ in range(fold)]
    if last:
        earlier = next(take)
    outs = [[next(take) for _ in pieces] for pieces in cuts]
    if last:
        ends = [next(take) for _ in range(2)]
    else:
        ends_all = next(take)
    parts = [next(take) for _ in range(2)]
    half = sizes[last]
    planes, cols = xs[1].shape[1:]
    lane = lax.broadcasted_iota(jnp.int32, (planes, LANES), 1)
    tiles = cols // LANES

    def fold_cell(j, _):
        for p in range(fold // 2):
            a, b = xs[p], xs[fold - 1 - p]
            for t in range(tiles):
                x = a[j + (at if p == 0 else 0), :, pl.ds(t * LANES, LANES)]
                y = b[j, :, pl.ds((tiles - 1 - t) * LANES, LANES)]
                y = lane_pick(y, LANES - 1 - lane)
                for parity in range(2):
                    v = x - y if parity else x + y
                    high = v.astype(BF16)
                    columns = pl.ds(p * cols + t * LANES, LANES)
                    place = pl.multiple_of(j * planes, planes)
                    parts[parity][pl.ds(place, planes), columns] = high
                    parts[parity][pl.ds(half * planes + place, planes), columns] = (v - high.astype(F32)).astype(BF16)
        return 0

    lax.fori_loop(0, half, fold_cell, 0)

    rows = half * planes
    modes = cols // 2
    wide = lax.broadcasted_iota(jnp.int32, (rows, LANES), 1)
    for r in range(fold):
        columns = pl.ds(r * modes, modes)
        sums = []
        for parity in range(2):
            dot = functools.partial(jnp.dot, preferred_element_type=F32)
            both = dot(parts[parity][...], tables[2 * parity][:, columns])
            rest = dot(parts[parity][:rows], tables[2 * parity + 1][:, columns])
            sums.append(both[:rows] + both[rows:] + rest)
        for t in range(tiles):
            source = slice((t // 2) * LANES, (t // 2 + 1) * LANES)
            index = wide // 2 + (t % 2) * (LANES // 2)
            even, odd = (lane_pick(s[:, source], index) for s in sums)
            tile = jnp.where(wide % 2 == 0, even, odd)
            tile = tile.reshape(half, planes, LANES)
            for out, (low, high) in zip(outs[r], cuts[r]):
                out[:, :, pl.ds(t * LANES, LANES)] = tile[low:high]

    for r in range(fold):
        for t in range(tiles):
            at_lanes = pl.ds(t * LANES, LANES)
            d = damp[r][:, at_lanes]
            w = weight_of(d)
            f = jnp.zeros_like(d)
            forward = []
            for out, (low, high) in zip(outs[r], cuts[r]):
                for j in range(high - low):
                    f = w * out[j, :, at_lanes] + d * f
                    forward.append(f)
            p = jnp.zeros_like(d)
            for j in reversed(range(half)):
                p = forward[j] + d * p
            if last:
                f0, p0 = earlier[0, r, :, at_lanes], earlier[1, r, :, at_lanes]
                f, p = merge((f, p), (f0, p0), idx[0] != 0, span(d, half), span(d, sizes[0]))
                ends[r % 2][r // 2, 0, :, at_lanes] = f
                ends[r % 2][r // 2, 1, :, at_lanes] = p
            else:
                ends_all[0, r, :, at_lanes] = f
                ends_all[1, r, :, at_lanes] = p


def transform(fold, sub, cuts, last, xs, tables, extra):
    planes, cols = xs[0].shape[1:]
    sizes = chunks(sub)
    half = sizes[last]
    at = sizes[0] if last else 0
    side = tables[0].shape[0]
    shape = lambda *n: jax.ShapeDtypeStruct(n, F32)
    outs = [shape(high - low, planes, cols) for pieces in cuts for low, high in pieces]
    if last:
        outs += [shape(fold // 2, 2, planes, cols)] * 2
    else:
        outs += [shape(2, fold, planes, cols)]
    rows = half * planes
    return pl.pallas_call(
        at_device(transform_kernel, fold, at, sizes, cuts, last),
        out_shape=outs,
        in_specs=vmem(len(xs) + 4 + len(extra)),
        out_specs=vmem(len(outs)),
        scratch_shapes=[pltpu.VMEM((2 * rows, side), BF16)] * 2,
        compiler_params=params(),
        cost_estimate=pl.CostEstimate(flops=12 * rows * side * side, bytes_accessed=8 * side * side, transcendentals=0),
        name="transform_b" if last else "transform_a",
    )(*xs, *tables, *extra)


def span(d, cells):
    power, gain, block = None, None, (d, d)
    while cells:
        if cells % 2:
            if power is None:
                power, gain = block
            else:
                power, gain = power * block[0], gain + power * power * block[1]
        block = doubled(*block)
        cells //= 2
    return power, gain


def merge(mine, other, upper, span_mine, span_other):
    pick = lambda a, b: a if a is b else jnp.where(upper, a, b)
    f_low, f_high = jnp.where(upper, other[0], mine[0]), jnp.where(upper, mine[0], other[0])
    p_low, p_high = jnp.where(upper, other[1], mine[1]), jnp.where(upper, mine[1], other[1])
    high_power, high_gain = pick(span_mine[0], span_other[0]), pick(span_mine[1], span_other[1])
    low_power = pick(span_other[0], span_mine[0])
    return f_high + high_power * f_low, p_low + low_power * (p_high + high_gain * f_low)


def doubled(power, gain):
    return power * power, gain * (1.0 + power * power)


def stages(count):
    bits = [1 << k for k in range(count.bit_length() - 1)]
    return [bits[k : k + 2] for k in range(0, len(bits), 2)]


def peers(bits):
    offsets = [0]
    for bit in bits:
        offsets += [o ^ bit for o in offsets]
    return offsets


def combine(groups, stage, d, block, row, ends, entry):
    power, gain = span(d, block)
    start, stop, turn = jnp.ones_like(d), jnp.ones_like(d), jnp.zeros_like(d)
    if entry is None:
        entry = (jnp.zeros_like(d), jnp.zeros_like(d))
    for k, bits in enumerate(groups[: stage + 1]):
        for bit in bits:
            upper = row & bit != 0
            if k == stage:
                mine, other = ends[0], ends[1]
                below, above = entry
                below = below + jnp.where(upper, start * other[0], 0.0)
                above = above + jnp.where(upper, turn * other[0], stop * (other[1] + gain * mine[0]))
                entry = (below, above)
                ends = [merge(ends[i], ends[i + 1], upper, (power, gain), (power, gain)) for i in range(0, len(ends), 2)]
            turn = jnp.where(upper, power * turn, turn + stop * gain * power)
            start = jnp.where(upper, power * start, start)
            stop = jnp.where(upper, stop, power * stop)
            power, gain = doubled(power, gain)
    return ends[0], entry


def combine_tiles(groups, stage, block, idx, damping, ends, entry, put):
    for t in range(damping.shape[1] // LANES):
        at = pl.ds(t * LANES, LANES)
        pairs = [(e[0, :, at], e[1, :, at]) for e in ends]
        entered = None if entry is None else (entry[0, :, at], entry[1, :, at])
        put(at, *combine(groups, stage, damping[:, at], block, idx[1], pairs, entered))


def combine_kernel(groups, stage, block, idx, damping, *refs):
    count = 1 << len(groups[stage])
    ends, rest = refs[:count], refs[count:]
    entry = rest[0] if stage else None
    outs = rest[-2:]

    def put(at, union, entered):
        outs[0][0, :, at], outs[0][1, :, at] = union
        outs[1][0, :, at], outs[1][1, :, at] = entered

    combine_tiles(groups, stage, block, idx, damping, ends, entry, put)


def combined(groups, stage, block, damping, ends, entry):
    pair = jax.ShapeDtypeStruct((2,) + damping.shape, F32)
    extra = [entry] if stage else []
    return pl.pallas_call(
        at_device(combine_kernel, groups, stage, block),
        out_shape=[pair, pair],
        in_specs=vmem(1 + len(ends) + len(extra)),
        out_specs=vmem(2),
        compiler_params=params(),
        cost_estimate=pl.CostEstimate(flops=100 * damping.size, bytes_accessed=32 * damping.size, transcendentals=0),
    )(damping, *ends, *extra)


def pairs_kernel(bit, sub, idx, keep, got, *refs):
    count = keep.shape[0]
    damp, outs = refs[:count], refs[count:]
    for i in range(count):
        for t in range(damp[i].shape[1] // LANES):
            at = pl.ds(t * LANES, LANES)
            both = span(damp[i][:, at], sub * bit)
            mine, other = ((e[i, 0, :, at], e[i, 1, :, at]) for e in (keep, got))
            out = outs[i % 2] if count > 1 else outs[0]
            place = (i // 2,) if count > 1 else ()
            f, p = merge(mine, other, idx[0] & bit != 0, both, both)
            out[(*place, 0, slice(None), at)] = f
            out[(*place, 1, slice(None), at)] = p


def block_ends(fold, sub, damp, keep, send):
    bit = 1
    while bit < fold:
        got = partner(send, "gy", bit)
        kept = [damp[r] for r in range(0, fold, 2 * bit)]
        count = len(kept)
        shape = keep.shape[1:] if count == 1 else (count // 2,) + keep.shape[1:]
        outs = [jax.ShapeDtypeStruct(shape, F32)] * (1 if count == 1 else 2)
        keep, *rest = pl.pallas_call(
            at_device(pairs_kernel, bit, sub),
            out_shape=outs,
            in_specs=vmem(2 + count),
            out_specs=vmem(len(outs)),
            compiler_params=params(),
            cost_estimate=pl.CostEstimate(flops=50 * keep.size, bytes_accessed=16 * keep.size, transcendentals=0),
        )(keep, got, *kept)
        send = rest[0] if rest else None
        bit *= 2
    return keep


def place(fold, cuts, me, sub):
    return [
        (chunk_start(me ^ r, h, sub) + low, high - low)
        for h in range(2)
        for r in range(fold)
        for low, high in cuts[h][r]
    ]


def gather_kernel(fold, cuts, chosen, idx, *refs):
    pieces, (gathered, out, sems) = refs[: len(chosen)], refs[len(chosen) :]
    places = place(fold, cuts, idx[0], gathered.shape[0] // fold)
    copies = []
    for n, k in enumerate(chosen):
        rows = pl.ds(*places[k])
        gathered[rows] = pieces[n][...]
        copies.append(pltpu.make_async_copy(gathered.at[rows], out.at[rows], sems.at[n]))
        copies[n].start()
    for copy in copies:
        copy.wait()


def gather(fold, cuts, pieces, chosen, shape):
    return pl.pallas_call(
        at_device(gather_kernel, fold, cuts, chosen),
        out_shape=[jax.ShapeDtypeStruct(shape, F32)] * 2,
        in_specs=vmem(len(chosen)),
        out_specs=vmem(1) + hbm(1),
        scratch_shapes=[pltpu.SemaphoreType.DMA((len(chosen),))],
        compiler_params=params(),
        cost_estimate=pl.CostEstimate(flops=math.prod(shape), bytes_accessed=8 * math.prod(shape), transcendentals=0),
        name="gather",
    )(*[pieces[k] for k in chosen])


def solve_kernel(fold, groups, cuts, chosen, idx, damping, *refs):
    stage = len(groups) - 1
    count = 1 << len(groups[stage])
    ends, rest = refs[:count], refs[count:]
    if stage:
        entry, rest = rest[0], rest[1:]
    else:
        entry = None
    pieces, rest = rest[: len(chosen)], rest[len(chosen) :]
    _, _, coefficients, coefficients_out, pressure_out, pressure, entered, c_sems, p_sems = rest
    cells = coefficients.shape[0]
    sub = cells // fold
    places = place(fold, cuts, idx[0], sub)
    copies = []
    for n, k in enumerate(chosen):
        rows = pl.ds(*places[k])
        coefficients[rows] = pieces[n][...]
        copies.append(pltpu.make_async_copy(coefficients.at[rows], coefficients_out.at[rows], c_sems.at[n]))
        copies[n].start()

    def put(at, union, entry):
        entered[0, :, at], entered[1, :, at] = entry

    combine_tiles(groups, stage, cells, idx, damping, ends, entry, put)
    width = max(coefficients.shape[2] // 2, LANES)
    for low in range(0, coefficients.shape[2], width):
        lanes = pl.ds(low, width)
        d = damping[:, lanes]
        w = weight_of(d)

        def forward(i, carry, w=w, d=d, lanes=lanes):
            f, now = carry
            following = coefficients[jnp.minimum(i + 1, cells - 1), :, lanes]
            f = w * now + d * f
            pressure[i, :, lanes] = f
            return f, following

        lax.fori_loop(0, cells, forward, (entered[0, :, lanes], coefficients[0, :, lanes]), unroll=8)

        p = entered[1, :, lanes]
        for block in reversed(range(fold)):

            def backward(i, p, d=d, lanes=lanes, block=block):
                at = (block + 1) * sub - 1 - i
                p = pressure[at, :, lanes] + d * p
                pressure[at, :, lanes] = p
                return p

            p = lax.fori_loop(0, sub, backward, p, unroll=8)
            part = (pl.ds(block * sub, sub), slice(None), lanes)
            k = len(copies) - len(chosen)
            copies.append(pltpu.make_async_copy(pressure.at[part], pressure_out.at[part], p_sems.at[k]))
            copies[-1].start()
    for copy in copies:
        copy.wait()


def solve(fold, groups, cuts, damping, ends, entry, pieces, chosen, gathered, partly):
    extra = [entry] if len(groups) > 1 else []
    operands = [damping, *ends, *extra, *[pieces[k] for k in chosen], gathered, partly]
    shape = jax.ShapeDtypeStruct(gathered.shape, F32)
    return pl.pallas_call(
        at_device(solve_kernel, fold, groups, cuts, chosen),
        out_shape=[shape] * 3,
        in_specs=vmem(len(operands) - 1) + hbm(1),
        out_specs=vmem(1) + hbm(2),
        scratch_shapes=[
            pltpu.VMEM(gathered.shape, F32),
            pltpu.VMEM((2,) + damping.shape, F32),
            pltpu.SemaphoreType.DMA((len(chosen),)),
            pltpu.SemaphoreType.DMA((2 * fold,)),
        ],
        input_output_aliases={len(operands) - 2: 0, len(operands) - 1: 1},
        compiler_params=params(),
        cost_estimate=pl.CostEstimate(flops=5 * gathered.size, bytes_accessed=12 * gathered.size, transcendentals=0),
        name="solve",
    )(*operands)[1:]


def body(velocity_u, wall_strain, damping):
    cells, planes, cols = velocity_u.shape
    fold = lax.axis_size("gy")
    sub = cells // fold
    order = list(range(fold - 1, 0, -1))
    first_send = first_cells(fold, velocity_u, wall_strain)
    *sends, near, far = lead(fold, velocity_u, wall_strain)
    sends.append(first_send)
    got = {(r, 0): partner(sends[r - 1], "gy", r) for r in order}
    near, far = exchange_edges(near, far)
    damp = {0: damping}
    bit = fold // 2
    while bit:
        damp |= {r ^ bit: partner(x, "gy", bit) for r, x in damp.items()}
        bit //= 2
    damp = [damp[r] for r in range(fold)]
    second, own, *sends = stencil(fold, velocity_u, wall_strain, near, far)
    for r in order:
        got[r, 1] = partner(sends[r - 1], "gy", r)
    tables = cosine_tables(fold, cols)
    cuts = pieces_of(fold, sub)
    first = transform(fold, sub, cuts[0], 0, [own] + [got[r, 0] for r in range(1, fold)], tables, damp)
    extra = [*damp, first[-1]]
    rest = transform(fold, sub, cuts[1], 1, [own] + [got[r, 1] for r in range(1, fold)], tables, extra)
    pieces = []
    for h, outs in enumerate((first, rest)):
        outs = iter(outs)
        for r in range(fold):
            for k in range(len(cuts[h][r])):
                out = next(outs)
                pieces.append(out if r == 0 else partner(out, "gy", r))
    groups = stages(lax.axis_size("gx"))
    mine, entry = block_ends(fold, sub, damp, *rest[-2:]), None
    for stage, bits in enumerate(groups):
        if stage:
            mine, entry = combined(groups, stage - 1, cells, damping, ends, entry)
        ends = [mine] + [partner(mine, "gx", o) for o in peers(bits)[1:]]
    late, k = [], 0
    for h in range(2):
        for r in range(fold):
            late += [k + n for n in range(len(cuts[h][r])) if h == 1 and r > 1]
            k += len(cuts[h][r])
    early = [n for n in range(k) if n not in late]
    gathered, partly = gather(fold, cuts, pieces, early, (cells, planes, cols))
    coefficients, pressure = solve(fold, groups, cuts, damping, ends, entry, pieces, late, gathered, partly)
    return second, coefficients, pressure


def pieces_of(fold, sub):
    return [[[(0, size)] for _ in range(fold)] for size in chunks(sub)]


def solution(mesh):
    return jax.shard_map(
        body,
        mesh=mesh,
        in_specs=(P("gx", None, "gy"), P("gx", None, "gy"), P(None, "gy")),
        out_specs=(P("gx", None, "gy"), P("gx", None, "gy"), P("gx", None, "gy")),
        check_vma=False,
    )
```

```python
import functools
import math

import jax
import jax.numpy as jnp
from jax import lax
from jax.experimental import pallas as pl
from jax.experimental.pallas import tpu as pltpu
from jax.sharding import PartitionSpec as P


LANES = 128
REACH = 3
F32 = jnp.float32
BF16 = jnp.bfloat16
MIB = 1024 * 1024
FIRST_LIMIT = 52 * MIB


def params(limit=16 * MIB):
    return pltpu.CompilerParams(vmem_limit_bytes=limit)


def vmem(count):
    return [pl.BlockSpec(memory_space=pltpu.VMEM)] * count


def at_device(kernel, *static):
    return lambda *refs: kernel(*static, (lax.axis_index("gy"), lax.axis_index("gx")), *refs)


def hbm(count):
    return [pl.BlockSpec(memory_space=pltpu.HBM)] * count


def partner(x, axis, bit):
    count = lax.axis_size(axis)
    return lax.ppermute(x, axis, [(i, i ^ bit) for i in range(count)])


def chunks(sub):
    later = max(5 * sub // 16, REACH)
    return sub - later, later


def chunk_start(block, h, sub):
    first, later = chunks(sub)
    return block * sub + (jnp.where(block == 0, later, 0) if h == 0 else jnp.where(block == 0, 0, first))


def derivatives(cell, at):
    c = [cell(at + k) for k in range(2 * REACH + 1)]
    first = 0.75 * (c[4] - c[2]) - 3.0 / 20.0 * (c[5] - c[1]) + 1.0 / 60.0 * (c[6] - c[0])
    second = (
        1.5 * (c[4] + c[2])
        - 3.0 / 20.0 * (c[5] + c[1])
        + 1.0 / 90.0 * (c[6] + c[0])
        - 49.0 / 18.0 * c[3]
    )
    return first, second


def first_kernel(fold, idx, u_in, wall_in, send, ubuf, wbuf, sems):
    size = send.shape[0]
    start = chunk_start(idx[0] ^ (fold - 1), 0, u_in.shape[0] // fold)
    u_copy = pltpu.make_async_copy(u_in.at[pl.ds(start - REACH, size + 2 * REACH)], ubuf, sems.at[0])
    w_copy = pltpu.make_async_copy(wall_in.at[pl.ds(start, size)], wbuf, sems.at[1])
    u_copy.start()
    w_copy.start()
    u_copy.wait()
    w_copy.wait()

    def step(j, _):
        first, _ = derivatives(lambda k: ubuf[k], j)
        send[j] = first + wbuf[j]
        return 0

    lax.fori_loop(0, size, step, 0, unroll=2)


def first_cells(fold, u, wall):
    cells, planes, cols = u.shape
    size = chunks(cells // fold)[0]
    return pl.pallas_call(
        at_device(first_kernel, fold),
        out_shape=jax.ShapeDtypeStruct((size, planes, cols), F32),
        in_specs=hbm(2),
        out_specs=vmem(1)[0],
        scratch_shapes=[
            pltpu.VMEM((size + 2 * REACH, planes, cols), F32),
            pltpu.VMEM((size, planes, cols), F32),
            pltpu.SemaphoreType.DMA((2,)),
        ],
        compiler_params=params(FIRST_LIMIT),
        cost_estimate=pl.CostEstimate(flops=size * planes * cols * 10, bytes_accessed=size * planes * cols * 12, transcendentals=0),
        name="first",
    )(u, wall)


def lead_kernel(fold, idx, u, wall, *refs):
    sends, (near, far) = refs[: fold - 2], refs[fold - 2 :]
    cells = u.shape[0]
    sub = cells // fold
    me, row = idx
    even = row % 2 == 0
    near[...] = u[pl.ds(jnp.where(even, cells - REACH, 0), REACH)]
    far[...] = u[pl.ds(jnp.where(even, 0, cells - REACH), REACH)]
    for r in range(fold - 2, 0, -1):
        start = chunk_start(me ^ r, 0, sub)

        def step(j, _, r=r, start=start):
            first, _ = derivatives(lambda k: u[k], start - REACH + j)
            sends[r - 1][j] = first + wall[start + j]
            return 0

        lax.fori_loop(0, chunks(sub)[0], step, 0, unroll=2)


def lead(fold, u, wall):
    cells, planes, cols = u.shape
    shape = lambda n: jax.ShapeDtypeStruct((n, planes, cols), F32)
    outs = [shape(chunks(cells // fold)[0])] * (fold - 2) + [shape(REACH)] * 2
    return pl.pallas_call(
        at_device(lead_kernel, fold),
        out_shape=outs,
        in_specs=vmem(2),
        out_specs=vmem(len(outs)),
        compiler_params=params(),
        cost_estimate=pl.CostEstimate(flops=cells * planes * cols * 6, bytes_accessed=cells * planes * cols * 6, transcendentals=0),
        name="lead",
    )(u, wall)


def stencil_kernel(fold, idx, u, wall, near, far, second_out, *refs):
    own, sends, (pad, second, out_sems) = refs[0], refs[1:fold], refs[fold:]
    cells = u.shape[0]
    sub = cells // fold
    sizes = chunks(sub)
    me = idx[0]
    even = idx[1] % 2 == 0
    pad[pl.ds(REACH, cells)] = u[...]
    pad[pl.ds(0, REACH)] = jnp.where(even, far[...], near[...])
    pad[pl.ds(REACH + cells, REACH)] = jnp.where(even, near[...], far[...])
    out_copies = []
    for r in range(fold - 1, -1, -1):
        block = me ^ r
        for h in (1, 0):
            start = chunk_start(block, h, sub)

            def step(j, _, r=r, h=h, start=start):
                first, second[start + j] = derivatives(lambda k: pad[k], start + j)
                if r == 0:
                    own[h * sizes[0] + j] = first + wall[start + j]
                elif h == 1:
                    sends[r - 1][j] = first + wall[start + j]
                return 0

            lax.fori_loop(0, sizes[h], step, 0, unroll=2)
        rows = pl.ds(block * sub, sub)
        copy = pltpu.make_async_copy(second.at[rows], second_out.at[rows], out_sems.at[r])
        copy.start()
        out_copies.append(copy)
    for copy in out_copies:
        copy.wait()


def stencil(fold, u, wall, near, far):
    cells, planes, cols = u.shape
    sub = cells // fold
    later = chunks(sub)[1]
    shape = lambda n: jax.ShapeDtypeStruct((n, planes, cols), F32)
    outs = [shape(cells), shape(sub)] + [shape(later)] * (fold - 1)
    return pl.pallas_call(
        at_device(stencil_kernel, fold),
        out_shape=outs,
        in_specs=vmem(4),
        out_specs=hbm(1) + vmem(len(outs) - 1),
        scratch_shapes=[
            pltpu.VMEM((cells + 2 * REACH, planes, cols), F32),
            pltpu.VMEM((cells, planes, cols), F32),
            pltpu.SemaphoreType.DMA((fold,)),
        ],
        compiler_params=params(),
        cost_estimate=pl.CostEstimate(flops=cells * planes * cols * 20, bytes_accessed=cells * planes * cols * 16, transcendentals=0),
        name="stencil",
    )(u, wall, near, far)


def exchange_edges(near, far):
    count = lax.axis_size("gx")
    inner = [(i, i + 1) for i in range(1, count - 1, 2)]
    far = lax.ppermute(far, "gx", inner + [(b, a) for a, b in inner])
    return partner(near, "gx", 1), far


def half_turn(phase, total):
    phase = phase - jnp.floor(phase * (1.0 / (4 * total))) * (4.0 * total)
    x = (jnp.abs(phase - 2.0 * total) - total) * (math.pi / (2.0 * total))
    s = x * x
    y = -1.0 / 39916800.0
    for coefficient in (1.0 / 362880.0, -1.0 / 5040.0, 1.0 / 120.0, -1.0 / 6.0, 1.0):
        y = y * s + coefficient
    return y * x


def table_kernel(total, cols, fold, chunk, idx, *outs):
    rows, width = outs[0].shape
    me = idx[0]
    modes = width // fold
    group = 8
    whole = lambda *shape: lambda axis: lax.broadcasted_iota(jnp.int32, shape, axis)
    base, inner, outer = whole(group, LANES), whole(chunk // group, LANES), whole(rows // chunk, LANES)
    at = outer(0) * chunk
    block = at // cols
    shifts = ((me ^ block) * cols + (at - block * cols)).astype(F32) * 2.0
    steps = (inner(0) * (2 * group)).astype(F32)
    sample = base(0).astype(F32) * 2.0 + 1.0

    def both(phase):
        return half_turn(phase, total), half_turn(phase - total, total)

    def column(c, _):
        r = c * LANES // modes
        first = (me ^ r) * modes + (c * LANES - r * modes)
        for parity in range(2):
            mode = lambda iota: (first + iota(1)).astype(F32) * 2.0 + parity
            c0, s0 = (v * math.sqrt(2.0 / total) for v in both(sample * mode(base)))
            ci, si = both(steps * mode(inner))
            co, so = both(shifts * mode(outer))
            cosine = jnp.concatenate([c0 * ci[i : i + 1] - s0 * si[i : i + 1] for i in range(chunk // group)])
            sine = jnp.concatenate([s0 * ci[i : i + 1] + c0 * si[i : i + 1] for i in range(chunk // group)])
            for i in range(rows // chunk):
                y = cosine * co[i : i + 1] - sine * so[i : i + 1]
                high = y.astype(BF16)
                place = (pl.ds(i * chunk, chunk), pl.ds(pl.multiple_of(c * LANES, LANES), LANES))
                outs[2 * parity][place] = high
                outs[2 * parity + 1][place] = (y - high.astype(F32)).astype(BF16)
        return 0

    lax.fori_loop(0, width // LANES, column, 0)


def cosine_tables(fold, cols):
    total = fold * cols
    side = total // 2
    return pl.pallas_call(
        at_device(table_kernel, total, cols, fold, 128),
        out_shape=[jax.ShapeDtypeStruct((side, side), BF16)] * 4,
        out_specs=vmem(4),
        compiler_params=params(),
        cost_estimate=pl.CostEstimate(flops=side * side * 60, bytes_accessed=side * side * 8, transcendentals=0),
        name="table",
    )()


def weight_of(d):
    t = (1.0 - d) * (1.0 + d)
    return t * jnp.sqrt(t)


def lane_pick(x, index):
    return jnp.take_along_axis(x, index, axis=1)


def transform_kernel(fold, at, sizes, cuts, last, idx, *refs):
    take = iter(refs)
    xs = [next(take) for _ in range(fold)]
    tables = [next(take) for _ in range(4)]
    damp = [next(take) for _ in range(fold)]
    if last:
        earlier = next(take)
    outs = [[next(take) for _ in pieces] for pieces in cuts]
    if last:
        ends = [next(take) for _ in range(2)]
    else:
        ends_all = next(take)
    parts = [next(take) for _ in range(2)]
    half = sizes[last]
    planes, cols = xs[1].shape[1:]
    lane = lax.broadcasted_iota(jnp.int32, (planes, LANES), 1)
    tiles = cols // LANES

    def fold_cell(j, _):
        for p in range(fold // 2):
            a, b = xs[p], xs[fold - 1 - p]
            for t in range(tiles):
                x = a[j + (at if p == 0 else 0), :, pl.ds(t * LANES, LANES)]
                y = b[j, :, pl.ds((tiles - 1 - t) * LANES, LANES)]
                y = lane_pick(y, LANES - 1 - lane)
                for parity in range(2):
                    v = x - y if parity else x + y
                    high = v.astype(BF16)
                    columns = pl.ds(p * cols + t * LANES, LANES)
                    place = pl.multiple_of(j * planes, planes)
                    parts[parity][pl.ds(place, planes), columns] = high
                    parts[parity][pl.ds(half * planes + place, planes), columns] = (v - high.astype(F32)).astype(BF16)
        return 0

    lax.fori_loop(0, half, fold_cell, 0)

    rows = half * planes
    modes = cols // 2
    wide = lax.broadcasted_iota(jnp.int32, (rows, LANES), 1)
    for r in range(fold):
        columns = pl.ds(r * modes, modes)
        sums = []
        for parity in range(2):
            dot = functools.partial(jnp.dot, preferred_element_type=F32)
            both = dot(parts[parity][...], tables[2 * parity][:, columns])
            rest = dot(parts[parity][:rows], tables[2 * parity + 1][:, columns])
            sums.append(both[:rows] + both[rows:] + rest)
        for t in range(tiles):
            source = slice((t // 2) * LANES, (t // 2 + 1) * LANES)
            index = wide // 2 + (t % 2) * (LANES // 2)
            even, odd = (lane_pick(s[:, source], index) for s in sums)
            tile = jnp.where(wide % 2 == 0, even, odd)
            tile = tile.reshape(half, planes, LANES)
            for out, (low, high) in zip(outs[r], cuts[r]):
                out[:, :, pl.ds(t * LANES, LANES)] = tile[low:high]

    for r in range(fold):
        for t in range(tiles):
            at_lanes = pl.ds(t * LANES, LANES)
            d = damp[r][:, at_lanes]
            w = weight_of(d)
            f = jnp.zeros_like(d)
            forward = []
            for out, (low, high) in zip(outs[r], cuts[r]):
                for j in range(high - low):
                    f = w * out[j, :, at_lanes] + d * f
                    forward.append(f)
            p = jnp.zeros_like(d)
            for j in reversed(range(half)):
                p = forward[j] + d * p
            if last:
                f0, p0 = earlier[0, r, :, at_lanes], earlier[1, r, :, at_lanes]
                f, p = merge((f, p), (f0, p0), idx[0] != 0, span(d, half), span(d, sizes[0]))
                ends[r % 2][r // 2, 0, :, at_lanes] = f
                ends[r % 2][r // 2, 1, :, at_lanes] = p
            else:
                ends_all[0, r, :, at_lanes] = f
                ends_all[1, r, :, at_lanes] = p


def transform(fold, sub, cuts, last, xs, tables, extra):
    planes, cols = xs[0].shape[1:]
    sizes = chunks(sub)
    half = sizes[last]
    at = sizes[0] if last else 0
    side = tables[0].shape[0]
    shape = lambda *n: jax.ShapeDtypeStruct(n, F32)
    outs = [shape(high - low, planes, cols) for pieces in cuts for low, high in pieces]
    if last:
        outs += [shape(fold // 2, 2, planes, cols)] * 2
    else:
        outs += [shape(2, fold, planes, cols)]
    rows = half * planes
    return pl.pallas_call(
        at_device(transform_kernel, fold, at, sizes, cuts, last),
        out_shape=outs,
        in_specs=vmem(len(xs) + 4 + len(extra)),
        out_specs=vmem(len(outs)),
        scratch_shapes=[pltpu.VMEM((2 * rows, side), BF16)] * 2,
        compiler_params=params(),
        cost_estimate=pl.CostEstimate(flops=12 * rows * side * side, bytes_accessed=8 * side * side, transcendentals=0),
        name="transform_b" if last else "transform_a",
    )(*xs, *tables, *extra)


def span(d, cells):
    power, gain, block = None, None, (d, d)
    while cells:
        if cells % 2:
            if power is None:
                power, gain = block
            else:
                power, gain = power * block[0], gain + power * power * block[1]
        block = doubled(*block)
        cells //= 2
    return power, gain


def merge(mine, other, upper, span_mine, span_other):
    pick = lambda a, b: a if a is b else jnp.where(upper, a, b)
    f_low, f_high = jnp.where(upper, other[0], mine[0]), jnp.where(upper, mine[0], other[0])
    p_low, p_high = jnp.where(upper, other[1], mine[1]), jnp.where(upper, mine[1], other[1])
    high_power, high_gain = pick(span_mine[0], span_other[0]), pick(span_mine[1], span_other[1])
    low_power = pick(span_other[0], span_mine[0])
    return f_high + high_power * f_low, p_low + low_power * (p_high + high_gain * f_low)


def doubled(power, gain):
    return power * power, gain * (1.0 + power * power)


def stages(count):
    bits = [1 << k for k in range(count.bit_length() - 1)]
    return [bits[k : k + 2] for k in range(0, len(bits), 2)]


def peers(bits):
    offsets = [0]
    for bit in bits:
        offsets += [o ^ bit for o in offsets]
    return offsets


def combine(groups, stage, d, block, row, ends, entry):
    power, gain = span(d, block)
    start, stop, turn = jnp.ones_like(d), jnp.ones_like(d), jnp.zeros_like(d)
    if entry is None:
        entry = (jnp.zeros_like(d), jnp.zeros_like(d))
    for k, bits in enumerate(groups[: stage + 1]):
        for bit in bits:
            upper = row & bit != 0
            if k == stage:
                mine, other = ends[0], ends[1]
                below, above = entry
                below = below + jnp.where(upper, start * other[0], 0.0)
                above = above + jnp.where(upper, turn * other[0], stop * (other[1] + gain * mine[0]))
                entry = (below, above)
                ends = [merge(ends[i], ends[i + 1], upper, (power, gain), (power, gain)) for i in range(0, len(ends), 2)]
            turn = jnp.where(upper, power * turn, turn + stop * gain * power)
            start = jnp.where(upper, power * start, start)
            stop = jnp.where(upper, stop, power * stop)
            power, gain = doubled(power, gain)
    return ends[0], entry


def combine_tiles(groups, stage, block, idx, damping, ends, entry, put):
    for t in range(damping.shape[1] // LANES):
        at = pl.ds(t * LANES, LANES)
        pairs = [(e[0, :, at], e[1, :, at]) for e in ends]
        entered = None if entry is None else (entry[0, :, at], entry[1, :, at])
        put(at, *combine(groups, stage, damping[:, at], block, idx[1], pairs, entered))


def combine_kernel(groups, stage, block, idx, damping, *refs):
    count = 1 << len(groups[stage])
    ends, rest = refs[:count], refs[count:]
    entry = rest[0] if stage else None
    final = stage == len(groups) - 1
    outs = rest[-1:] if final else rest[-2:]

    def put(at, union, entered):
        if not final:
            outs[1][0, :, at], outs[1][1, :, at] = union
        outs[0][0, :, at], outs[0][1, :, at] = entered

    combine_tiles(groups, stage, block, idx, damping, ends, entry, put)


def combined(groups, stage, block, damping, ends, entry):
    pair = jax.ShapeDtypeStruct((2,) + damping.shape, F32)
    extra = [entry] if stage else []
    outs = [pair] if stage == len(groups) - 1 else [pair, pair]
    return pl.pallas_call(
        at_device(combine_kernel, groups, stage, block),
        out_shape=outs,
        in_specs=vmem(1 + len(ends) + len(extra)),
        out_specs=vmem(len(outs)),
        compiler_params=params(),
        cost_estimate=pl.CostEstimate(flops=100 * damping.size, bytes_accessed=32 * damping.size, transcendentals=0),
    )(damping, *ends, *extra)


def pairs_kernel(bit, sub, idx, keep, got, *refs):
    count = keep.shape[0]
    damp, outs = refs[:count], refs[count:]
    for i in range(count):
        for t in range(damp[i].shape[1] // LANES):
            at = pl.ds(t * LANES, LANES)
            both = span(damp[i][:, at], sub * bit)
            mine, other = ((e[i, 0, :, at], e[i, 1, :, at]) for e in (keep, got))
            out = outs[i % 2] if count > 1 else outs[0]
            place = (i // 2,) if count > 1 else ()
            f, p = merge(mine, other, idx[0] & bit != 0, both, both)
            out[(*place, 0, slice(None), at)] = f
            out[(*place, 1, slice(None), at)] = p


def block_ends(fold, sub, damp, keep, send):
    bit = 1
    while bit < fold:
        got = partner(send, "gy", bit)
        kept = [damp[r] for r in range(0, fold, 2 * bit)]
        count = len(kept)
        shape = keep.shape[1:] if count == 1 else (count // 2,) + keep.shape[1:]
        outs = [jax.ShapeDtypeStruct(shape, F32)] * (1 if count == 1 else 2)
        keep, *rest = pl.pallas_call(
            at_device(pairs_kernel, bit, sub),
            out_shape=outs,
            in_specs=vmem(2 + count),
            out_specs=vmem(len(outs)),
            compiler_params=params(),
            cost_estimate=pl.CostEstimate(flops=50 * keep.size, bytes_accessed=16 * keep.size, transcendentals=0),
        )(keep, got, *kept)
        send = rest[0] if rest else None
        bit *= 2
    return keep


def place(fold, cuts, me, sub):
    return [
        (chunk_start(me ^ r, h, sub) + low, high - low)
        for h in range(2)
        for r in range(fold)
        for low, high in cuts[h][r]
    ]


def gather_kernel(fold, cuts, chosen, idx, *refs):
    pieces, (gathered, out, sems) = refs[: len(chosen)], refs[len(chosen) :]
    places = place(fold, cuts, idx[0], gathered.shape[0] // fold)
    copies = []
    for n, k in enumerate(chosen):
        rows = pl.ds(*places[k])
        gathered[rows] = pieces[n][...]
        copies.append(pltpu.make_async_copy(gathered.at[rows], out.at[rows], sems.at[n]))
        copies[n].start()
    for copy in copies:
        copy.wait()


def gather(fold, cuts, pieces, chosen, shape):
    return pl.pallas_call(
        at_device(gather_kernel, fold, cuts, chosen),
        out_shape=[jax.ShapeDtypeStruct(shape, F32)] * 2,
        in_specs=vmem(len(chosen)),
        out_specs=vmem(1) + hbm(1),
        scratch_shapes=[pltpu.SemaphoreType.DMA((len(chosen),))],
        compiler_params=params(),
        cost_estimate=pl.CostEstimate(flops=math.prod(shape), bytes_accessed=8 * math.prod(shape), transcendentals=0),
        name="gather",
    )(*[pieces[k] for k in chosen])


def solve_kernel(fold, cuts, chosen, idx, damping, entered, *refs):
    pieces, rest = refs[: len(chosen)], refs[len(chosen) :]
    _, _, coefficients, coefficients_out, pressure_out, pressure, c_sems, p_sems = rest
    cells = coefficients.shape[0]
    sub = cells // fold
    places = place(fold, cuts, idx[0], sub)
    copies = []
    for n, k in enumerate(chosen):
        rows = pl.ds(*places[k])
        coefficients[rows] = pieces[n][...]
        copies.append(pltpu.make_async_copy(coefficients.at[rows], coefficients_out.at[rows], c_sems.at[n]))
        copies[n].start()

    width = max(coefficients.shape[2] // 2, LANES)
    for low in range(0, coefficients.shape[2], width):
        lanes = pl.ds(low, width)
        d = damping[:, lanes]
        w = weight_of(d)

        def forward(i, carry, w=w, d=d, lanes=lanes):
            f, now = carry
            following = coefficients[jnp.minimum(i + 1, cells - 1), :, lanes]
            f = w * now + d * f
            pressure[i, :, lanes] = f
            return f, following

        lax.fori_loop(0, cells, forward, (entered[0, :, lanes], coefficients[0, :, lanes]), unroll=8)

        p = entered[1, :, lanes]
        for block in reversed(range(fold)):

            def backward(i, p, d=d, lanes=lanes, block=block):
                at = (block + 1) * sub - 1 - i
                p = pressure[at, :, lanes] + d * p
                pressure[at, :, lanes] = p
                return p

            p = lax.fori_loop(0, sub, backward, p, unroll=8)
            part = (pl.ds(block * sub, sub), slice(None), lanes)
            k = len(copies) - len(chosen)
            copies.append(pltpu.make_async_copy(pressure.at[part], pressure_out.at[part], p_sems.at[k]))
            copies[-1].start()
    for copy in copies:
        copy.wait()


def solve(fold, cuts, damping, entered, pieces, chosen, gathered, partly):
    operands = [damping, entered, *[pieces[k] for k in chosen], gathered, partly]
    shape = jax.ShapeDtypeStruct(gathered.shape, F32)
    return pl.pallas_call(
        at_device(solve_kernel, fold, cuts, chosen),
        out_shape=[shape] * 3,
        in_specs=vmem(len(operands) - 1) + hbm(1),
        out_specs=vmem(1) + hbm(2),
        scratch_shapes=[
            pltpu.VMEM(gathered.shape, F32),
            pltpu.SemaphoreType.DMA((len(chosen),)),
            pltpu.SemaphoreType.DMA((2 * fold,)),
        ],
        input_output_aliases={len(operands) - 2: 0, len(operands) - 1: 1},
        compiler_params=params(),
        cost_estimate=pl.CostEstimate(flops=5 * gathered.size, bytes_accessed=12 * gathered.size, transcendentals=0),
        name="solve",
    )(*operands)[1:]


def body(velocity_u, wall_strain, damping):
    cells, planes, cols = velocity_u.shape
    fold = lax.axis_size("gy")
    sub = cells // fold
    order = list(range(fold - 1, 0, -1))
    first_send = first_cells(fold, velocity_u, wall_strain)
    *sends, near, far = lead(fold, velocity_u, wall_strain)
    sends.append(first_send)
    got = {(r, 0): partner(sends[r - 1], "gy", r) for r in order}
    near, far = exchange_edges(near, far)
    damp = {0: damping}
    bit = fold // 2
    while bit:
        damp |= {r ^ bit: partner(x, "gy", bit) for r, x in damp.items()}
        bit //= 2
    damp = [damp[r] for r in range(fold)]
    second, own, *sends = stencil(fold, velocity_u, wall_strain, near, far)
    for r in order:
        got[r, 1] = partner(sends[r - 1], "gy", r)
    tables = cosine_tables(fold, cols)
    cuts = pieces_of(fold, sub)
    first = transform(fold, sub, cuts[0], 0, [own] + [got[r, 0] for r in range(1, fold)], tables, damp)
    extra = [*damp, first[-1]]
    rest = transform(fold, sub, cuts[1], 1, [own] + [got[r, 1] for r in range(1, fold)], tables, extra)
    pieces = []
    for h, outs in enumerate((first, rest)):
        outs = iter(outs)
        for r in range(fold):
            for k in range(len(cuts[h][r])):
                out = next(outs)
                pieces.append(out if r == 0 else partner(out, "gy", r))
    groups = stages(lax.axis_size("gx"))
    mine, entry = block_ends(fold, sub, damp, *rest[-2:]), None
    for stage, bits in enumerate(groups):
        if stage:
            entry, mine = combined(groups, stage - 1, cells, damping, ends, entry)
        ends = [mine] + [partner(mine, "gx", o) for o in peers(bits)[1:]]
    (entered,) = combined(groups, len(groups) - 1, cells, damping, ends, entry)
    late, k = [], 0
    for h in range(2):
        for r in range(fold):
            late += [k + n for n in range(len(cuts[h][r])) if h == 1 and r > 1]
            k += len(cuts[h][r])
    early = [n for n in range(k) if n not in late]
    gathered, partly = gather(fold, cuts, pieces, early, (cells, planes, cols))
    coefficients, pressure = solve(fold, cuts, damping, entered, pieces, late, gathered, partly)
    return second, coefficients, pressure


def pieces_of(fold, sub):
    return [[[(0, size)] for _ in range(fold)] for size in chunks(sub)]


def solution(mesh):
    return jax.shard_map(
        body,
        mesh=mesh,
        in_specs=(P("gx", None, "gy"), P("gx", None, "gy"), P(None, "gy")),
        out_specs=(P("gx", None, "gy"), P("gx", None, "gy"), P("gx", None, "gy")),
        check_vma=False,
    )
```
